32 devices in a mesh: groups: 2 (over y), ep: 16 (over z, x, core).
Axes of the slice: x: 2, y: 2, z: 4, core: 2. Of those that a mesh axis runs over, the one named last changes fastest.
Arguments:
- tokens: bfloat16 [4096, 1440], P(('groups', 'ep')), parts along dimension 0, may hold values from -6 to 6
- expert_ids: int32 [4096, 4], P(('groups', 'ep')), parts along dimension 0, may hold values from 0 to 15, as said below
- combine: float32 [4096, 4], P(('groups', 'ep')), parts along dimension 0, may hold values from 0.05 to 1
- gate_weight: bfloat16 [16, 1440, 1440], P('ep'), may hold values from -0.15625 to 0.15625
- up_weight: bfloat16 [16, 1440, 1440], P('ep'), may hold values from -0.15625 to 0.15625
- down_weight: bfloat16 [16, 1440, 1440], P('ep'), may hold values from -0.15625 to 0.15625
Outputs:
- mixture: bfloat16 [4096, 1440], P(('groups', 'ep')), parts along dimension 0
The draws below stay inside these ranges and needn't reach their ends.
There are 2 independent parts, one for each index of `groups`. The reference program is written for one: setup_inputs(seed, part) draws one part's arguments, and reference() takes and returns one part's arrays. A program takes and returns all parts, laid end to end along the dimension named above; an argument that names none is the same for every part. Nothing has to cross between parts.
Inputs may be any that keep to these rules, and one draw needn't show every extreme that they name: `expert_ids`: each row names 4 different experts. In the rows of one device (aligned blocks of 128 rows) no expert is named more than 64 times, and some expert is named exactly 64 times in every block.
All inputs are finite; a program needn't handle non-finite values.
Results may differ from the reference program's by a relative error of at most 0.0058.
Values may be sent and summed in bfloat16 or wider, within the bound.
A program may use at most 64 MiB of HBM per device.

```python
import math
import jax
import jax.numpy as jnp
from jax import lax

D = 1440
FF = 1440
TOP = 4
TOK_DEV = 128
EXPERTS = 16
TOKENS = 2048
CAP = 64
N_EP = 16


def route_block(key, ranking):
    cells = EXPERTS * CAP
    expert_of_cell = jnp.arange(cells, dtype=jnp.int32) // CAP
    position_in_expert = ranking[expert_of_cell]
    routing_boost = (4 << 20) // (position_in_expert + 1)
    random_jitter = jax.random.randint(jax.random.fold_in(key, 1), (cells,), 0, 1 << 20, dtype=jnp.int32)
    router_logits = routing_boost + random_jitter
    chosen = jnp.argsort(-router_logits, stable=True)[:TOK_DEV * TOP]
    listed = jnp.sort(expert_of_cell[chosen])
    table = listed.reshape(TOP, TOK_DEV).T
    random_reorder = jax.random.permutation(jax.random.fold_in(key, 2), TOK_DEV)
    return table[random_reorder]


def draw_expert_ids(key, part):
    ranking = jax.random.permutation(jax.random.fold_in(key, 7), EXPERTS).astype(jnp.int32)

    def one_block(index):
        return route_block(jax.random.fold_in(key, 100 + index), ranking)
    blocks = jax.vmap(one_block)(jnp.arange(N_EP, dtype=jnp.int32))
    return blocks.reshape(TOKENS, TOP).astype(jnp.int32)


def steps_of(own_key, dims, split, low, top_value):
    def one(axis_at, blocks):
        draws = jax.random.uniform(jax.random.fold_in(jax.random.fold_in(own_key, 6), axis_at), (blocks,), jnp.float32, low / len(split), top_value / len(split))
        return jnp.repeat(jnp.exp(draws), dims[axis_at] // blocks).reshape((-1,) + (1,) * (len(dims) - axis_at - 1))

    level = one(*split[0])
    for cut in split[1:]:
        level = level * one(*cut)
    return level


def bell_draw(key, extent, spread, reach, cuts=(), kind=jnp.bfloat16):
    entries = spread * jax.random.normal(key, extent, jnp.float32)
    if cuts:
        entries = entries * steps_of(key, extent, cuts, -0.22, 0.18)
    return jnp.clip(entries, -reach, reach).astype(kind)


def setup_inputs(seed: int = 0, part: int = 0) -> dict:
    arg_keys = jax.random.split(jax.random.key(seed), 7)
    own_keys = jax.random.split(jax.random.fold_in(arg_keys[6], part), 7)
    tokens = bell_draw(own_keys[0], (TOKENS, D), 1.0, 6.0, ((0, 16),))
    expert_ids = draw_expert_ids(jax.random.fold_in(jax.random.fold_in(arg_keys[6], part), 71), part)
    combine = jnp.clip(jnp.exp(math.log(1.0) - 2.9957323 * jax.random.uniform(own_keys[2], (TOKENS, TOP), jnp.float32) ** steps_of(own_keys[2], (TOKENS, TOP), ((0, 16),), -0.2, 0.2)), 0.05, 1.0)
    gate_weight = bell_draw(arg_keys[3], (EXPERTS, D, FF), D ** -0.5, 0.15625, ((0, 16),))
    up_weight = bell_draw(arg_keys[4], (EXPERTS, D, FF), D ** -0.5, 0.15625, ((0, 16),))
    down_weight = bell_draw(arg_keys[5], (EXPERTS, FF, D), FF ** -0.5, 0.15625, ((0, 16),))
    return dict(tokens=tokens, expert_ids=expert_ids, combine=combine, gate_weight=gate_weight, up_weight=up_weight, down_weight=down_weight)


alpha_gate = 1.702


def run_expert_block(row_block, gate_proj, up_proj, down_proj):
    gate_part = jnp.dot(row_block, gate_proj, preferred_element_type=jnp.float32)
    up_part = jnp.dot(row_block, up_proj, preferred_element_type=jnp.float32)
    hidden = ((up_part + 1.0) * gate_part * jax.nn.sigmoid(alpha_gate * gate_part)).astype(jnp.bfloat16)
    return jnp.dot(hidden, down_proj, preferred_element_type=jnp.float32).astype(jnp.bfloat16)


def reference(tokens, expert_ids, combine, gate_weight, up_weight, down_weight):
    most_rows = N_EP * CAP

    def per_expert(carry, inputs):
        expert, gate_proj, up_proj, down_proj = inputs
        chosen = expert_ids == expert
        weight_row = jnp.sum(jnp.where(chosen, combine, jnp.zeros_like(combine)), axis=1)
        present = jnp.any(chosen, axis=1)
        indices = jnp.nonzero(present, size=most_rows, fill_value=0)[0].astype(jnp.int32)
        valid = jnp.arange(most_rows, dtype=jnp.int32) < jnp.sum(present.astype(jnp.int32))
        outputs = run_expert_block(tokens[indices], gate_proj, up_proj, down_proj)
        factor = jnp.where(valid, weight_row[indices], jnp.zeros_like(weight_row[indices]))
        rescaled_logits = outputs.astype(jnp.float32) * factor[:, None]
        return carry.at[indices].add(rescaled_logits), None

    total = jnp.zeros(tokens.shape, jnp.float32)
    total, unused = lax.scan(per_expert, total, (jnp.arange(EXPERTS, dtype=jnp.int32), gate_weight, up_weight, down_weight))
    return total.astype(jnp.bfloat16)
```

```python
import functools

import jax
import jax.numpy as jnp
from jax import lax
from jax.experimental import pallas as pl
from jax.experimental.pallas import tpu as pltpu
from jax.sharding import PartitionSpec as P

MESH = pl.DeviceIdType.MESH

alpha_gate = 1.702

SHARES = ((0.0, 0.0, 0.0), (0.67, 0.34, 0.34), 1.0, False)
CHUNKS = (2.4, 1.2)
HOP, ACROSS_CHIP, BLOCK = 1.8, 1.7, 8.0


def run_expert_block(row_block, gate_proj, up_proj, down_proj):
    gate_part = jnp.dot(row_block, gate_proj, preferred_element_type=jnp.float32)
    up_part = jnp.dot(row_block, up_proj, preferred_element_type=jnp.float32)
    hidden = ((up_part + 1.0) * gate_part * jax.nn.sigmoid(alpha_gate * gate_part)).astype(
        jnp.bfloat16
    )
    return jnp.dot(hidden, down_proj, preferred_element_type=jnp.float32).astype(jnp.bfloat16)


class Routes:
    def __init__(self, length, pieces, twin_share, both_share, first=1.0, hold=False):
        self.length, self.pieces = length, pieces
        self.half = (length + 1) // 2
        self.twin_share, self.both_share = twin_share, both_share
        self.first, self.hold = round(first * pieces), hold

    def twin(self, distance, p):
        share = self.twin_share[min(distance, len(self.twin_share)) - 1]
        return p < round(share * self.pieces)

    def both(self, chain, q):
        share = self.both_share[min(chain, len(self.both_share)) - 1]
        return q < round(share * self.pieces)

    def chain(self, u, d):
        return u if d > 0 else self.length - 1 - u

    def exists(self, w, d):
        return 0 <= w + d < self.length

    def late(self, w, p):
        return p >= self.first and w > 0 and w + 1 < self.length

    def neighbour(self, w, d):
        to = w + d
        return (to, False) if to < self.half else (self.length - 1 - to, True)

    def token_moves(self, w, u, col, p):
        if u == w:
            if col == 0:
                out = (1,) if self.late(w, p) else (1, -1)
                return tuple(d for d in out if self.exists(w, d)), True
            return tuple(d for d in (1, -1) if self.exists(w, d) and self.twin(1, p)), False
        d, far = (1, w - u) if u < w else (-1, u - w)
        onward = self.exists(w, d)
        if col == 0:
            return ((d,) if onward else ()), not self.twin(far, p)
        if not self.twin(far, p):
            return (), False
        return ((d,) if onward and self.twin(far + 1, p) else ()), False

    def sum_inputs(self, kind, w, u, col, q):
        if kind == "X":
            return (), False
        if kind == "Z":
            d = 1 if u > w else -1
            return ((d,) if self.exists(w, -d) else ()), not self.both(self.chain(u, d), q)
        chains = tuple(
            d for d in (1, -1)
            if self.exists(w, -d) and (col == 0 or self.both(self.chain(w, d), q))
        )
        return chains, col == 0


def make_plan(routes):
    length, pieces, half = routes.length, routes.pieces, routes.half
    never = 1e9
    wire = BLOCK / pieces
    link, tok, pair_in, ans, cross, chain = {}, {}, {}, {}, {}, {}
    done_at = [dict() for _ in range(half)]

    def push(w, name, now):
        start = max(now, link.get((w, name), 0.0))
        link[w, name] = start + wire
        return start + wire + HOP

    def send_tokens(w, u, col, p, now):
        moves, crosses = routes.token_moves(w, u, col, p)
        for d in moves:
            to, mirrored = routes.neighbour(w, d)
            tok[to, length - 1 - u if mirrored else u, col, p] = push(w, d, now)
        if crosses:
            tok[w, u, 1 - col, p] = push(w, 0, now)
        key = (w, u, col)
        pair_in.setdefault(key, {})[p] = now + ACROSS_CHIP

    def send_sum(kind, w, u, col, q, now):
        if kind == "X" or (kind == "F" and col == 1):
            cross[w, u, q] = push(w, 0, now)
        elif kind == "Z":
            d = 1 if u > w else -1
            to, mirrored = routes.neighbour(w, d)
            key = (to, -d, length - 1 - u) if mirrored else (to, d, u)
            chain[key + (col, q)] = push(w, d, now)

    todo = []
    for w in range(half):
        ops = []
        for u in range(length):
            for col in range(2):
                if (u, col) == (w, 0):
                    ops += [("o", u, 0, p) for p in range(pieces) if routes.late(w, p)]
                else:
                    ops += [("t", u, col, p) for p in range(pieces)]
            for q in range(pieces):
                if u == w:
                    ops += [("F", u, 1, q), ("F", u, 0, q)]
                elif routes.both(routes.chain(u, 1 if u > w else -1), q):
                    ops += [("Z", u, 0, q), ("Z", u, 1, q)]
                else:
                    ops += [("X", u, 1, q), ("Z", u, 0, q)]
        todo.append(ops)

    def ready_at(w, op):
        kind, u, col, p = op
        if kind == "t":
            return tok.get((w, u, col, p), never)
        if kind == "o":
            return never if any(o[:3] == ("t", length - 1, 0) for o in todo[w]) else 0.0
        if routes.hold and (kind == "X" or (kind == "F" and col == 1)) and any(
            o[0] == "t" for o in todo[w]
        ):
            return never
        at = ans.get((w, u, col), never)
        chains, crossing = routes.sum_inputs(kind, w, u, col, p)
        for d in chains:
            at = max(at, chain.get((w, d, u, col, p), never))
        if crossing:
            at = max(at, cross.get((w, u, p), never))
        return at

    rank = {"t": 0, "o": 0, "X": 1, "Z": 2, "F": 3}
    pairs = [
        sorted(((u, col) for u in range(length) for col in range(2)),
               key=lambda k: (abs(k[0] - w), k[1], k[0]))
        for w in range(half)
    ]
    order = [[] for _ in range(half)]
    slots = [{} for _ in range(half)]
    busy = [0.0] * half
    at_slot = [(0, 0)] * half
    running = [None] * half
    for w in range(half):
        for p in range(pieces):
            send_tokens(w, w, 0, p, 0.0)
    steps = 2 * length
    tick, now, end = 0.05, 0.0, [0.0] * half
    while now < 1000 and any(todo):
        for w in range(half):
            if busy[w] > now:
                continue
            if running[w] is not None:
                u, col = running[w]
                ans[w, u, col] = now + ACROSS_CHIP
                running[w] = None
            open_ops, held = [], set()
            for op in todo[w]:
                lane = op[:3]
                if lane in held:
                    continue
                if ready_at(w, op) <= now:
                    open_ops.append(op)
                elif op[0] == "t":
                    held.add(lane)
            i, j = at_slot[w]
            if open_ops:
                op = min(open_ops, key=lambda o: (rank[o[0]], abs(o[1] - w), o[1], o[2], o[3]))
                todo[w].remove(op)
                slots[w].setdefault((i, j), []).append(op)
                kind = op[0]
                busy[w] = now + (0.05 if kind in "to" else 0.4 / pieces + 0.05)
                if kind == "t":
                    send_tokens(w, *op[1:], now)
                elif kind == "o":
                    to, mirrored = routes.neighbour(w, -1)
                    tok[to, length - 1 - w if mirrored else w, 0, op[3]] = push(w, -1, now)
                else:
                    send_sum(kind, w, *op[1:], busy[w])
                end[w] = busy[w]
                continue
            if i < steps:
                if j == 0:
                    got = [
                        k for k in pairs[w]
                        if len(pair_in.get((w,) + k, {})) == pieces
                        and max(pair_in[(w,) + k].values()) <= now
                    ]
                    if not got or now < 2.5:
                        continue
                    pairs[w].remove(got[0])
                    order[w].append(got[0])
                busy[w] = now + CHUNKS[j]
                if j + 1 == len(CHUNKS):
                    running[w] = order[w][-1]
                    at_slot[w] = (i + 1, 0)
                else:
                    at_slot[w] = (i, j + 1)
        now += tick
    return order, slots, end


def grouped(routes, w, ops):
    groups = []
    for kind, u, col, p in ops:
        if kind == "o":
            how = ((-1,), False)
        elif kind == "t":
            how = routes.token_moves(w, u, col, p)
        else:
            how = routes.sum_inputs(kind, w, u, col, p)
        if groups and groups[-1][:4] == [kind, u, col, how] and groups[-1][5] == p:
            groups[-1][5] = p + 1
        else:
            groups.append([kind, u, col, how, p, p + 1])
    return groups


def exchange_kernel(
    ids_ref, share_ref, tok_hbm, gate_hbm, up_hbm, down_hbm, out_ref,
    x_buf, w_out, w_in, rank_buf, gate_w, up_w, down_w, hid, sums, quad, over, flow,
    load_sem, x_s, xp_s, w_s, q_s, sum_s, x_r, xp_r, w_r, q_r, over_r, flow_r,
    *, members, capacity, routes,
):
    length, pieces, half = routes.length, routes.pieces, routes.half
    order, slots, _ = make_plan(routes)
    features, here = tok_hbm.shape
    size = features // pieces
    me = lax.axis_index("ep")
    z, x, c = me // 4, (me // 2) % 2, me % 2
    flip = 2 * z >= length
    at = jnp.where(flip, length - 1 - z, z)

    def member(zz, xx, cc):
        return (zz * 2 + xx) * 2 + cc

    across, partner = member(z, 1 - x, c), member(z, x, 1 - c)
    step_up = jnp.where(flip, -1, 1)

    def beside(d):
        return member(jnp.clip(z + d * step_up, 0, length - 1), x, c)

    def lane(d):
        return jnp.where(flip, 1, 0) if d > 0 else jnp.where(flip, 0, 1)

    def place(u):
        return jnp.where(flip, length - 1 - u, u)

    def column(col):
        return x if col == 0 else 1 - x

    def cut(p, count=1):
        return pl.ds(pl.multiple_of(p * size, size), count * size)

    def send(src, dst, ssem, rsem, to):
        return pltpu.make_async_remote_copy(
            src_ref=src, dst_ref=dst, send_sem=ssem, recv_sem=rsem,
            device_id={"ep": to}, device_id_type=MESH,
        )

    def each(p0, p1, act):
        if p1 - p0 == 1:
            act(p0)
            return

        def one(p, carry):
            act(p)
            return carry

        lax.fori_loop(p0, p1, one, 0)

    loads = [
        pltpu.make_async_copy(tok_hbm, x_buf.at[z, x, c], load_sem.at[0]),
        pltpu.make_async_copy(gate_hbm, gate_w, load_sem.at[1]),
        pltpu.make_async_copy(up_hbm, up_w, load_sem.at[2]),
        pltpu.make_async_copy(down_hbm, down_w, load_sem.at[3]),
    ]
    for load in loads:
        load.start()

    barrier = pltpu.get_barrier_semaphore()
    for step in range(1, members):
        to = lax.rem(me + step, members)
        pl.semaphore_signal(barrier, inc=1, device_id={"ep": to}, device_id_type=MESH)

    expert = lax.broadcasted_iota(jnp.int32, (members, here), 0)
    mix = jnp.zeros((members, here), jnp.float32)
    for k in range(ids_ref.shape[0]):
        mix += jnp.where(ids_ref[k : k + 1, :] == expert, share_ref[k : k + 1, :], 0.0)
    for e in range(members):
        w_out[e] = mix[e : e + 1, :]
    pl.semaphore_wait(barrier, members - 1)

    def weights_copy(step):
        to = lax.rem(me + step, members)
        return send(w_out.at[to], w_in.at[me], w_s.at[step], w_r.at[me], to)

    def weights_arrival(step):
        origin = lax.rem(me + step, members)
        return send(w_out.at[origin], w_in.at[origin], w_s.at[step], w_r.at[origin], origin)

    sent = [[] for _ in range(half)]

    def token_copy(zz, xx, p, way, count=1):
        slot = x_buf.at[zz, xx, c, cut(p, count)]
        number, to = (2, across) if way == 0 else (lane(way), beside(way))
        return send(slot, slot, x_s.at[zz, xx, number], x_r.at[zz, xx, p], to)

    def partner_copy(zz, xx, p=None):
        slot = x_buf.at[zz, xx, c] if p is None else x_buf.at[zz, xx, c, cut(p)]
        return send(slot, slot, xp_s.at[zz, xx], xp_r.at[zz, xx], partner)

    def move_tokens(w, u, col, how, p0, p1, arriving, share=True):
        zz, xx = place(u), column(col)
        ways = tuple(how[0]) + ((0,) if how[1] else ())

        def one(p):
            if arriving:
                token_copy(zz, xx, p, 0).wait_recv()
            for way in ways:
                token_copy(zz, xx, p, way).start()
            if share:
                partner_copy(zz, xx, p).start()

        each(p0, p1, one)
        for way in ways:
            sent[w].append(("t", u, col, way, p1 - p0))

    joins = [{} for _ in range(half)]
    for w in range(half):
        for slot in sorted(slots[w]):
            for kind, u, col, q in slots[w][slot]:
                if kind in "XZF":
                    joins[w].setdefault((u, col), (kind, q))

    def answer_copy(zz, xx):
        return send(
            sums.at[zz, xx, 1 - c], quad.at[zz, xx], q_s.at[zz, xx], q_r.at[zz, xx], partner
        )

    def over_copy(zz, xx, q, count=1):
        return send(
            sums.at[zz, xx, c, cut(q, count)], over.at[zz, cut(q, count)],
            sum_s.at[zz, xx, 0], over_r.at[zz, q], across,
        )

    def flow_copy(zz, xx, q, way, count=1):
        d = lane(way)
        return send(
            sums.at[zz, xx, c, cut(q, count)], flow.at[d, zz, xx, cut(q, count)],
            sum_s.at[zz, xx, 1], flow_r.at[d, zz, xx, q], beside(way),
        )

    def move_sums(kind, w, u, col, how, q0, q1):
        zz, xx = place(u), column(col)
        chains, crossing = how
        if joins[w][u, col] == (kind, q0):
            answer_copy(zz, xx).wait_recv()
        leaves = kind == "X" or (kind == "F" and col == 1)
        onward = 1 if u > w else -1

        def one(q):
            for d in chains:
                flow_copy(zz, xx, q, d).wait_recv()
            if crossing:
                over_copy(zz, xx, q).wait_recv()
            total = sums[zz, xx, c, cut(q)].astype(jnp.float32)
            total += quad[zz, xx, cut(q)].astype(jnp.float32)
            if crossing:
                total += over[zz, cut(q)].astype(jnp.float32)
            for d in chains:
                total += flow[lane(d), zz, xx, cut(q)].astype(jnp.float32)
            total = total.astype(jnp.bfloat16)
            if kind == "F" and col == 0:
                out_ref[cut(q), :] = total
                return
            sums[zz, xx, c, cut(q)] = total
            if leaves:
                over_copy(zz, xx, q).start()
            else:
                flow_copy(zz, xx, q, onward).start()

        each(q0, q1, one)
        if leaves:
            sent[w].append(("x", u, col, 0, q1 - q0))
        elif kind == "Z":
            sent[w].append(("z", u, col, onward, q1 - q0))

    def run_slot(i, j):
        for w in range(half):
            due = [(k, slots[w][k, j]) for k in range(2 * length + 1) if (k, j) in slots[w]]
            due = [(k, ops) for k, ops in due if (k == 2 * length) == (i is None)]
            if not due:
                continue

            @pl.when(at == w)
            def _(w=w, due=due):
                for k, ops in due:

                    def act(ops=ops):
                        for kind, u, col, how, p0, p1 in grouped(routes, w, ops):
                            if kind == "t":
                                move_tokens(w, u, col, how, p0, p1, True)
                            elif kind == "o":
                                move_tokens(w, u, col, how, p0, p1, False, False)
                            else:
                                move_sums(kind, w, u, col, how, p0, p1)

                    if i is None:
                        act()
                    else:
                        pl.when(i == k)(act)

    for step in range(1, members):
        weights_copy(step).start()
    loads[0].wait()
    for w in range(half):

        @pl.when(at == w)
        def _(w=w):
            for _, u, col, how, p0, p1 in grouped(
                routes, w, [("t", w, 0, p) for p in range(pieces)]
            ):
                move_tokens(w, u, col, how, p0, p1, False)

    w_in[me] = w_out[me]
    before = (
        lax.broadcasted_iota(jnp.int32, (here, here), 0)
        < lax.broadcasted_iota(jnp.int32, (here, here), 1)
    ).astype(jnp.bfloat16)
    for step in range(1, members):
        weights_arrival(step).wait_recv()
    weight = jnp.concatenate([w_in[e] for e in range(members)], axis=0)
    named = weight > 0.0
    rank = jnp.dot(
        named.astype(jnp.float32).astype(jnp.bfloat16), before,
        preferred_element_type=jnp.float32,
    )
    rank = jnp.where(named, rank, -1.0)
    for e in range(members):
        rank_buf[e] = rank[e : e + 1, :]
    row_at = lax.broadcasted_iota(jnp.int32, (capacity, here), 0).astype(jnp.float32)

    def pickers(zz, xx):
        picks = []
        for cc in range(2):
            e = member(zz, xx, cc)
            pick = rank_buf[e] == row_at
            picks.append((
                pick.astype(jnp.float32).astype(jnp.bfloat16),
                jnp.where(pick, w_in[e], 0.0).astype(jnp.bfloat16),
            ))
        none = jnp.zeros((capacity, here), jnp.bfloat16)

        def spread(k):
            first = jnp.concatenate([picks[0][k], none], axis=1)
            second = jnp.concatenate([none, picks[1][k]], axis=1)
            return jnp.concatenate([first, second], axis=0)

        return spread(0), spread(1)

    def inner(zz, xx):
        pick, _ = pickers(zz, xx)
        pair = jnp.concatenate([x_buf[zz, xx, 0], x_buf[zz, xx, 1]], axis=1)
        block = lax.dot_general(
            pick, pair, (((1,), (1,)), ((), ())), preferred_element_type=jnp.float32
        ).astype(jnp.bfloat16)
        gate = jnp.dot(block, gate_w[...], preferred_element_type=jnp.float32)
        up = jnp.dot(block, up_w[...], preferred_element_type=jnp.float32)
        hid[...] = ((up + 1.0) * gate * jax.nn.sigmoid(alpha_gate * gate)).astype(jnp.bfloat16)

    def outer(zz, xx):
        _, mixer = pickers(zz, xx)
        answer = jnp.dot(
            hid[...], down_w[...], preferred_element_type=jnp.float32
        ).astype(jnp.bfloat16)
        back = lax.dot_general(
            answer, mixer, (((0,), (0,)), ((), ())), preferred_element_type=jnp.float32
        ).astype(jnp.bfloat16)
        for cc in range(2):
            sums[zz, xx, cc] = back[:, cc * here : (cc + 1) * here]

    def lookup(i, k):
        value = 0
        for w in range(half):
            for n in range(2 * length):
                here_now = jnp.logical_and(at == w, i == n)
                value = jnp.where(here_now, order[w][n][k], value)
        return value

    for load in loads[1:]:
        load.wait()

    def step_of(i, carry):
        run_slot(i, 0)
        zz = place(lookup(i, 0))
        xx = (x + lookup(i, 1)) % 2
        partner_copy(zz, xx).wait_recv()
        inner(zz, xx)
        run_slot(i, 1)
        outer(zz, xx)
        answer_copy(zz, xx).start()
        return carry

    lax.fori_loop(0, 2 * length, step_of, 0)
    run_slot(None, 0)

    for step in range(1, members):
        weights_copy(step).wait_send()
    for w in range(half):

        @pl.when(at == w)
        def _(w=w):
            counts = {}
            for kind, u, col, way, n in sent[w]:
                counts[kind, u, col, way] = counts.get((kind, u, col, way), 0) + n
            for (kind, u, col, way), n in counts.items():
                zz, xx = place(u), column(col)
                if kind == "t":
                    token_copy(zz, xx, 0, way, n).wait_send()
                elif kind == "x":
                    over_copy(zz, xx, 0, n).wait_send()
                else:
                    flow_copy(zz, xx, 0, way, n).wait_send()

    def drain(zz, carry):
        for xx in range(2):
            partner_copy(zz, xx).wait_send()
            answer_copy(zz, xx).wait_send()
        return carry

    lax.fori_loop(0, length, drain, 0)


def gathered_plan(tokens, expert_ids, combine, gate_proj, up_proj, down_proj, capacity):
    members = lax.axis_size("ep")
    here, features = tokens.shape
    ff = gate_proj.shape[1]
    length = members // 4
    pieces = max(n for n in range(1, 7) if features % (16 * n) == 0)
    routes = Routes(length, pieces, *SHARES)
    block = (features, here)
    dma = pltpu.SemaphoreType.DMA
    vmem = lambda *shape: pltpu.VMEM(shape, jnp.bfloat16)
    anywhere = pl.BlockSpec(memory_space=pl.ANY)
    inside = pl.BlockSpec(memory_space=pltpu.VMEM)
    return pl.pallas_call(
        functools.partial(
            exchange_kernel, members=members, capacity=capacity, routes=routes
        ),
        out_shape=jax.ShapeDtypeStruct(block, jnp.bfloat16),
        in_specs=[inside, inside, anywhere, anywhere, anywhere, anywhere],
        out_specs=inside,
        scratch_shapes=[
            vmem(length, 2, 2, *block),
            pltpu.VMEM((members, 1, here), jnp.float32),
            pltpu.VMEM((members, 1, here), jnp.float32),
            pltpu.VMEM((members, 1, here), jnp.float32),
            vmem(features, ff), vmem(features, ff), vmem(ff, features),
            vmem(2 * capacity, ff),
            vmem(length, 2, 2, *block), vmem(length, 2, *block),
            vmem(length, *block), vmem(2, length, 2, *block),
            dma((4,)), dma((length, 2, 3)), dma((length, 2)), dma((members,)),
            dma((length, 2)), dma((length, 2, 2)),
            dma((length, 2, pieces)), dma((length, 2)), dma((members,)), dma((length, 2)),
            dma((length, pieces)), dma((2, length, 2, pieces)),
        ],
        compiler_params=pltpu.CompilerParams(
            collective_id=0, has_side_effects=True, vmem_limit_bytes=60 * 1024 * 1024
        ),
    )(expert_ids.T, combine.T, tokens.T, gate_proj, up_proj, down_proj).T


def on_device(tokens, expert_ids, combine, gate_weight, up_weight, down_weight):
    members = lax.axis_size("ep")
    tokens_here, fanout = expert_ids.shape
    features = tokens.shape[1]
    capacity = 2 * tokens_here * fanout // members
    received_rows = members * capacity
    if members % 4 == 0 and 2 * capacity >= tokens_here:
        return gathered_plan(
            tokens, expert_ids, combine, gate_weight[0], up_weight[0], down_weight[0], capacity
        )
    flat_ids = expert_ids.reshape(-1)
    onehot = (flat_ids[:, None] == jnp.arange(members, dtype=jnp.int32)[None, :]).astype(jnp.int32)
    running = jnp.cumsum(onehot, axis=0) - onehot
    slot_rank = jnp.sum(running * onehot, axis=1)
    target = flat_ids * capacity + slot_rank
    source_token = jnp.arange(tokens_here * fanout, dtype=jnp.int32) // fanout
    outgoing = (
        jnp.zeros((received_rows, features), jnp.bfloat16).at[target].set(tokens[source_token])
    )
    outgoing = outgoing.reshape(members, capacity, features)
    gate_proj, up_proj, down_proj = (gate_weight[0], up_weight[0], down_weight[0])
    arrived = lax.all_to_all(outgoing, "ep", split_axis=0, concat_axis=0, tiled=True)
    shape_here = arrived.shape
    answers = run_expert_block(
        arrived.reshape(-1, features), gate_proj, up_proj, down_proj
    ).reshape(shape_here)
    returned = lax.all_to_all(answers, "ep", split_axis=0, concat_axis=0, tiled=True)
    selected_experts = (
        returned.reshape(-1, features)[target]
        .astype(jnp.float32)
        .reshape(tokens_here, fanout, features)
    )
    mixture = jnp.sum(selected_experts * combine[:, :, None], axis=1)
    return mixture.astype(jnp.bfloat16)


def solution(mesh):
    in_specs = (
        P(("groups", "ep"), None),
        P(("groups", "ep"), None),
        P(("groups", "ep"), None),
        P("ep", None, None),
        P("ep", None, None),
        P("ep", None, None),
    )
    out_specs = P(("groups", "ep"), None)
    return jax.shard_map(
        on_device, mesh=mesh, in_specs=in_specs, out_specs=out_specs, check_vma=False
    )
```

```python
import functools

import jax
import jax.numpy as jnp
from jax import lax
from jax.experimental import pallas as pl
from jax.experimental.pallas import tpu as pltpu
from jax.sharding import PartitionSpec as P

MESH = pl.DeviceIdType.MESH

alpha_gate = 1.702

PIECES = 6
TWIN, NEAR = ((0.83, 0.5, 0.17), (0.17, 0), (0,)), ((0.67, 0.33, 0.33), (0.67, 0.67), (0,))
ORDER = ((1.0, 0.33), 1, True, ((15, 10), (0, 15)), ((0, 4, 1, 2, 3, 6, 5, 7), (2, 3, 0, 4, 1, 5, 7, 6)), ((4, 3, 1, 1, 2, 2, 3, 0), (2, 1, 4, 3, 1, 1, 2, 2)))
CHUNKS = (1.8, 0.9)
HOP, ACROSS_CHIP, BLOCK = 2.4, 1.6, 8.0


def run_expert_block(row_block, gate_proj, up_proj, down_proj):
    gate_part = jnp.dot(row_block, gate_proj, preferred_element_type=jnp.float32)
    up_part = jnp.dot(row_block, up_proj, preferred_element_type=jnp.float32)
    hidden = ((up_part + 1.0) * gate_part * jax.nn.sigmoid(alpha_gate * gate_part)).astype(
        jnp.bfloat16
    )
    return jnp.dot(hidden, down_proj, preferred_element_type=jnp.float32).astype(jnp.bfloat16)


class Routes:
    def __init__(self, length, pieces, twin, near, first, crossing, far, after, pairs, urgency):
        self.length, self.pieces = length, pieces
        self.half = (length + 1) // 2
        self.shares = twin, near
        self.first, self.crossing, self.far = first, crossing, far
        self.after, self.pairs, self.urgency = after, pairs, urgency

    def within(self, which, u, w, distance, p):
        if u >= self.half:
            u, w = self.length - 1 - u, self.length - 1 - w
        kind = 0 if u == 0 else 1 if w > u else 2
        shares = self.shares[which][kind]
        return p < shares[min(distance, len(shares)) - 1] * self.pieces - 0.5

    def twin(self, u, w, distance, p):
        return self.within(0, u, w, distance, p)

    def near(self, u, w, distance, q):
        return self.within(1, u, w, distance, q)

    def exists(self, w, d):
        return 0 <= w + d < self.length

    def late(self, w, p, d):
        share = self.first[d < 0]
        return p >= share * self.pieces - 0.5 and w > 0 and w + 1 < self.length

    def crosses_late(self, p):
        return p >= self.crossing * self.pieces - 0.5

    def neighbour(self, w, d):
        to = w + d
        return (to, False) if to < self.half else (self.length - 1 - to, True)

    def token_moves(self, w, u, col, p):
        if u == w:
            ways = tuple(d for d in (1, -1) if self.exists(w, d))
            if col == 0:
                early = tuple(d for d in ways if not self.late(w, p, d))
                return early, not self.crosses_late(p)
            return tuple(d for d in ways if self.twin(w, w + d, 1, p)), False
        d, far = (1, w - u) if u < w else (-1, u - w)
        onward = self.exists(w, d)
        if col == 0:
            return ((d,) if onward else ()), not self.twin(u, w, far, p)
        if not self.twin(u, w, far, p):
            return (), False
        return ((d,) if onward and self.twin(u, w, far + 1, p) else ()), False

    def sum_inputs(self, kind, w, u, col, q):
        if kind == "X":
            return (), False
        if kind == "Z":
            d, away = (1, u - w) if u > w else (-1, w - u)
            chains = self.exists(w, -d) and (col == 0 or self.near(u, w, away + 1, q))
            return ((d,) if chains else ()), not self.near(u, w, away, q)
        chains = tuple(
            d for d in (1, -1)
            if self.exists(w, -d) and (col == 0 or self.near(w, w - d, 1, q))
        )
        return chains, col == 0


def make_plan(routes):
    length, pieces, half = routes.length, routes.pieces, routes.half
    never = 1e9
    wire = BLOCK / pieces
    link, tok, pair_in, ans, cross, chain = {}, {}, {}, {}, {}, {}
    done_at = [dict() for _ in range(half)]

    def push(w, name, now):
        start = max(now, link.get((w, name), 0.0))
        link[w, name] = start + wire
        return start + wire + HOP

    def send_tokens(w, u, col, p, now):
        moves, crosses = routes.token_moves(w, u, col, p)
        for d in moves:
            to, mirrored = routes.neighbour(w, d)
            tok[to, length - 1 - u if mirrored else u, col, p] = push(w, d, now)
        if crosses:
            tok[w, u, 1 - col, p] = push(w, 0, now)
        key = (w, u, col)
        pair_in.setdefault(key, {})[p] = now + ACROSS_CHIP

    def send_sum(kind, w, u, col, q, now):
        if kind == "X" or (kind == "F" and col == 1):
            cross[w, u, q] = push(w, 0, now)
        elif kind == "Z":
            d = 1 if u > w else -1
            to, mirrored = routes.neighbour(w, d)
            key = (to, -d, length - 1 - u) if mirrored else (to, d, u)
            chain[key + (col, q)] = push(w, d, now)

    todo = []
    for w in range(half):
        ops = []
        for u in range(length):
            for col in range(2):
                if (u, col) == (w, 0):
                    ops += [("o", u, 0, p) for p in range(pieces) if routes.late(w, p, -1)]
                    ops += [("v", u, 0, p) for p in range(pieces) if routes.late(w, p, 1)]
                    ops += [("c", u, 0, p) for p in range(pieces) if routes.crosses_late(p)]
                else:
                    ops += [("t", u, col, p) for p in range(pieces)]
            for q in range(pieces):
                if u == w:
                    ops += [("F", u, 1, q), ("F", u, 0, q)]
                elif routes.near(u, w, abs(u - w), q):
                    ops += [("Z", u, 0, q), ("Z", u, 1, q)]
                else:
                    ops += [("X", u, 1, q), ("Z", u, 0, q)]
        todo.append(ops)

    def ready_at(w, op):
        kind, u, col, p = op
        if kind == "t":
            return tok.get((w, u, col, p), never)
        if kind == "o":
            return never if any(o[:3] == ("t", length - 1, 0) for o in todo[w]) else 0.0
        if kind == "v":
            return never if any(o[0] == "t" and o[1] < w and o[2] == 0 for o in todo[w]) else 0.0
        if kind == "c":
            waiting = any(
                o[0] == "t" and routes.token_moves(w, *o[1:])[1] for o in todo[w]
            )
            return never if waiting else 0.0
        at = ans.get((w, u, col), never)
        if kind == "X" or (kind == "F" and col == 1):
            at = max(at, routes.after[w][kind == "F"])
        chains, crossing = routes.sum_inputs(kind, w, u, col, p)
        for d in chains:
            at = max(at, chain.get((w, d, u, col, p), never))
        if crossing:
            at = max(at, cross.get((w, u, p), never))
        return at

    pairs = []
    for w in range(half):
        wanted = sorted(
            ((u, col) for u in range(length) for col in range(2)),
            key=lambda k: (abs(k[0] - w), k[1], k[0]),
        )
        if length == len(routes.pairs[w]) // 2:
            wanted = [(n // 2, n % 2) for n in routes.pairs[w]]
        pairs.append(wanted)

    def precedence(w, op):
        kind, u, col, p = op
        if kind in "tocv":
            return -1, (-1 if routes.far else 1) * abs(u - w), u, col, p
        n = 2 * u + col
        rank = routes.urgency[w][n] if 2 * length == len(routes.urgency[w]) else abs(u - w)
        return rank, kind != "X", u, col, p

    order = [[] for _ in range(half)]
    slots = [{} for _ in range(half)]
    busy = [0.0] * half
    at_slot = [(0, 0)] * half
    running = [None] * half
    for w in range(half):
        for p in range(pieces):
            send_tokens(w, w, 0, p, 0.0)
    steps = 2 * length
    tick, now, end = 0.1, 0.0, [0.0] * half
    while now < 1000 and any(todo):
        for w in range(half):
            if busy[w] > now:
                continue
            if running[w] is not None:
                u, col = running[w]
                ans[w, u, col] = now + ACROSS_CHIP
                running[w] = None
            open_ops, held = [], set()
            for op in todo[w]:
                lane = op[:3]
                if lane in held:
                    continue
                if ready_at(w, op) <= now:
                    open_ops.append(op)
                elif op[0] == "t":
                    held.add(lane)
            i, j = at_slot[w]
            if open_ops:
                op = min(open_ops, key=lambda o: precedence(w, o))
                todo[w].remove(op)
                slots[w].setdefault((i, j), []).append(op)
                kind = op[0]
                busy[w] = now + (0.05 if kind in "tocv" else 0.4 / pieces + 0.05)
                if kind == "t":
                    send_tokens(w, *op[1:], now)
                elif kind in "ov":
                    way = -1 if kind == "o" else 1
                    to, mirrored = routes.neighbour(w, way)
                    tok[to, length - 1 - w if mirrored else w, 0, op[3]] = push(w, way, now)
                elif kind == "c":
                    tok[w, w, 1, op[3]] = push(w, 0, now)
                else:
                    send_sum(kind, w, *op[1:], busy[w])
                end[w] = busy[w]
                continue
            if i < steps:
                if j == 0:
                    got = [
                        k for k in pairs[w]
                        if len(pair_in.get((w,) + k, {})) == pieces
                        and max(pair_in[(w,) + k].values()) <= now
                    ]
                    if not got or now < 2.5:
                        continue
                    pairs[w].remove(got[0])
                    order[w].append(got[0])
                busy[w] = now + CHUNKS[j]
                if j + 1 == len(CHUNKS):
                    running[w] = order[w][-1]
                    at_slot[w] = (i + 1, 0)
                else:
                    at_slot[w] = (i, j + 1)
        now += tick
    return order, slots, end


def grouped(routes, w, ops):
    groups = []
    for kind, u, col, p in ops:
        if kind in "ocv":
            how = {"o": ((-1,), False), "v": ((1,), False), "c": ((), True)}[kind]
        elif kind == "t":
            how = routes.token_moves(w, u, col, p)
        else:
            how = routes.sum_inputs(kind, w, u, col, p)
        if groups and groups[-1][:4] == [kind, u, col, how] and groups[-1][5] == p:
            groups[-1][5] = p + 1
        else:
            groups.append([kind, u, col, how, p, p + 1])
    return groups


def exchange_kernel(
    ids_ref, share_ref, tok_hbm, gate_hbm, up_hbm, down_hbm, out_ref,
    x_buf, w_out, w_in, rank_buf, gate_w, up_w, down_w, hid, sums, quad, over, flow,
    load_sem, x_s, xp_s, w_s, q_s, sum_s, x_r, xp_r, w_r, q_r, over_r, flow_r,
    *, members, capacity, routes,
):
    length, pieces, half = routes.length, routes.pieces, routes.half
    order, slots, _ = make_plan(routes)
    features, here = tok_hbm.shape
    size = features // pieces
    me = lax.axis_index("ep")
    z, x, c = me // 4, (me // 2) % 2, me % 2
    flip = 2 * z >= length
    at = jnp.where(flip, length - 1 - z, z)

    def member(zz, xx, cc):
        return (zz * 2 + xx) * 2 + cc

    across, partner = member(z, 1 - x, c), member(z, x, 1 - c)
    step_up = jnp.where(flip, -1, 1)

    def beside(d):
        return member(jnp.clip(z + d * step_up, 0, length - 1), x, c)

    def lane(d):
        return jnp.where(flip, 1, 0) if d > 0 else jnp.where(flip, 0, 1)

    def place(u):
        return jnp.where(flip, length - 1 - u, u)

    def column(col):
        return x if col == 0 else 1 - x

    def cut(p, count=1):
        return pl.ds(pl.multiple_of(p * size, size), count * size)

    def send(src, dst, ssem, rsem, to):
        return pltpu.make_async_remote_copy(
            src_ref=src, dst_ref=dst, send_sem=ssem, recv_sem=rsem,
            device_id={"ep": to}, device_id_type=MESH,
        )

    def each(p0, p1, act):
        if p1 - p0 == 1:
            act(p0)
            return

        def one(p, carry):
            act(p)
            return carry

        lax.fori_loop(p0, p1, one, 0)

    loads = [
        pltpu.make_async_copy(tok_hbm, x_buf.at[z, x, c], load_sem.at[0]),
        pltpu.make_async_copy(gate_hbm, gate_w, load_sem.at[1]),
        pltpu.make_async_copy(up_hbm, up_w, load_sem.at[2]),
        pltpu.make_async_copy(down_hbm, down_w, load_sem.at[3]),
    ]
    for load in loads:
        load.start()

    barrier = pltpu.get_barrier_semaphore()
    for step in range(1, members):
        to = lax.rem(me + step, members)
        pl.semaphore_signal(barrier, inc=1, device_id={"ep": to}, device_id_type=MESH)

    expert = lax.broadcasted_iota(jnp.int32, (members, here), 0)
    mix = jnp.zeros((members, here), jnp.float32)
    for k in range(ids_ref.shape[0]):
        mix += jnp.where(ids_ref[k : k + 1, :] == expert, share_ref[k : k + 1, :], 0.0)
    for e in range(members):
        w_out[e] = mix[e : e + 1, :]
    pl.semaphore_wait(barrier, members - 1)

    def weights_copy(step):
        to = lax.rem(me + step, members)
        return send(w_out.at[to], w_in.at[me], w_s.at[step], w_r.at[me], to)

    def weights_arrival(step):
        origin = lax.rem(me + step, members)
        return send(w_out.at[origin], w_in.at[origin], w_s.at[step], w_r.at[origin], origin)

    sent = [[] for _ in range(half)]

    def token_copy(zz, xx, p, way, count=1):
        slot = x_buf.at[zz, xx, c, cut(p, count)]
        number, to = (2, across) if way == 0 else (lane(way), beside(way))
        return send(slot, slot, x_s.at[zz, xx, number], x_r.at[zz, xx, p], to)

    def partner_copy(zz, xx, p=None):
        slot = x_buf.at[zz, xx, c] if p is None else x_buf.at[zz, xx, c, cut(p)]
        return send(slot, slot, xp_s.at[zz, xx], xp_r.at[zz, xx], partner)

    def move_tokens(w, u, col, how, p0, p1, arriving, share=True):
        zz, xx = place(u), column(col)
        ways = tuple(how[0]) + ((0,) if how[1] else ())

        def one(p):
            if arriving:
                token_copy(zz, xx, p, 0).wait_recv()
            for way in ways:
                token_copy(zz, xx, p, way).start()
            if share:
                partner_copy(zz, xx, p).start()

        each(p0, p1, one)
        for way in ways:
            sent[w].append(("t", u, col, way, p1 - p0))

    joins = [{} for _ in range(half)]
    for w in range(half):
        for slot in sorted(slots[w]):
            for kind, u, col, q in slots[w][slot]:
                if kind in "XZF":
                    joins[w].setdefault((u, col), (kind, q))

    def answer_copy(zz, xx):
        return send(
            sums.at[zz, xx, 1 - c], quad.at[zz, xx], q_s.at[zz, xx], q_r.at[zz, xx], partner
        )

    def over_copy(zz, xx, q, count=1):
        return send(
            sums.at[zz, xx, c, cut(q, count)], over.at[zz, cut(q, count)],
            sum_s.at[zz, xx, 0], over_r.at[zz, q], across,
        )

    def flow_copy(zz, xx, q, way, count=1):
        d = lane(way)
        return send(
            sums.at[zz, xx, c, cut(q, count)], flow.at[d, zz, xx, cut(q, count)],
            sum_s.at[zz, xx, 1], flow_r.at[d, zz, xx, q], beside(way),
        )

    def move_sums(kind, w, u, col, how, q0, q1):
        zz, xx = place(u), column(col)
        chains, crossing = how
        if joins[w][u, col] == (kind, q0):
            answer_copy(zz, xx).wait_recv()
        leaves = kind == "X" or (kind == "F" and col == 1)
        onward = 1 if u > w else -1

        def one(q):
            for d in chains:
                flow_copy(zz, xx, q, d).wait_recv()
            if crossing:
                over_copy(zz, xx, q).wait_recv()
            total = sums[zz, xx, c, cut(q)].astype(jnp.float32)
            total += quad[zz, xx, cut(q)].astype(jnp.float32)
            if crossing:
                total += over[zz, cut(q)].astype(jnp.float32)
            for d in chains:
                total += flow[lane(d), zz, xx, cut(q)].astype(jnp.float32)
            total = total.astype(jnp.bfloat16)
            if kind == "F" and col == 0:
                out_ref[cut(q), :] = total
                return
            sums[zz, xx, c, cut(q)] = total
            if leaves:
                over_copy(zz, xx, q).start()
            else:
                flow_copy(zz, xx, q, onward).start()

        each(q0, q1, one)
        if leaves:
            sent[w].append(("x", u, col, 0, q1 - q0))
        elif kind == "Z":
            sent[w].append(("z", u, col, onward, q1 - q0))

    def run_slot(i, j):
        for w in range(half):
            due = [(k, slots[w][k, j]) for k in range(2 * length + 1) if (k, j) in slots[w]]
            due = [(k, ops) for k, ops in due if (k == 2 * length) == (i is None)]
            if not due:
                continue

            @pl.when(at == w)
            def _(w=w, due=due):
                for k, ops in due:

                    def act(ops=ops):
                        for kind, u, col, how, p0, p1 in grouped(routes, w, ops):
                            if kind == "t":
                                move_tokens(w, u, col, how, p0, p1, True)
                            elif kind in "ocv":
                                move_tokens(w, u, col, how, p0, p1, False, False)
                            else:
                                move_sums(kind, w, u, col, how, p0, p1)

                    if i is None:
                        act()
                    else:
                        pl.when(i == k)(act)

    for step in range(1, members):
        weights_copy(step).start()
    loads[0].wait()
    for w in range(half):

        @pl.when(at == w)
        def _(w=w):
            for _, u, col, how, p0, p1 in grouped(
                routes, w, [("t", w, 0, p) for p in range(pieces)]
            ):
                move_tokens(w, u, col, how, p0, p1, False)

    w_in[me] = w_out[me]
    before = (
        lax.broadcasted_iota(jnp.int32, (here, here), 0)
        < lax.broadcasted_iota(jnp.int32, (here, here), 1)
    ).astype(jnp.bfloat16)
    for step in range(1, members):
        weights_arrival(step).wait_recv()
    weight = jnp.concatenate([w_in[e] for e in range(members)], axis=0)
    named = weight > 0.0
    rank = jnp.dot(
        named.astype(jnp.float32).astype(jnp.bfloat16), before,
        preferred_element_type=jnp.float32,
    )
    rank = jnp.where(named, rank, -1.0)
    for e in range(members):
        rank_buf[e] = rank[e : e + 1, :]
    row_at = lax.broadcasted_iota(jnp.int32, (capacity, here), 0).astype(jnp.float32)

    def pickers(zz, xx):
        picks = []
        for cc in range(2):
            e = member(zz, xx, cc)
            pick = rank_buf[e] == row_at
            picks.append((
                pick.astype(jnp.float32).astype(jnp.bfloat16),
                jnp.where(pick, w_in[e], 0.0).astype(jnp.bfloat16),
            ))
        none = jnp.zeros((capacity, here), jnp.bfloat16)

        def spread(k):
            first = jnp.concatenate([picks[0][k], none], axis=1)
            second = jnp.concatenate([none, picks[1][k]], axis=1)
            return jnp.concatenate([first, second], axis=0)

        return spread(0), spread(1)

    def inner(zz, xx):
        pick, _ = pickers(zz, xx)
        pair = jnp.concatenate([x_buf[zz, xx, 0], x_buf[zz, xx, 1]], axis=1)
        block = lax.dot_general(
            pick, pair, (((1,), (1,)), ((), ())), preferred_element_type=jnp.float32
        ).astype(jnp.bfloat16)
        gate = jnp.dot(block, gate_w[...], preferred_element_type=jnp.float32)
        up = jnp.dot(block, up_w[...], preferred_element_type=jnp.float32)
        hid[...] = ((up + 1.0) * gate * jax.nn.sigmoid(alpha_gate * gate)).astype(jnp.bfloat16)

    def outer(zz, xx):
        _, mixer = pickers(zz, xx)
        answer = jnp.dot(
            hid[...], down_w[...], preferred_element_type=jnp.float32
        ).astype(jnp.bfloat16)
        back = lax.dot_general(
            answer, mixer, (((0,), (0,)), ((), ())), preferred_element_type=jnp.float32
        ).astype(jnp.bfloat16)
        for cc in range(2):
            sums[zz, xx, cc] = back[:, cc * here : (cc + 1) * here]

    def lookup(i, k):
        value = 0
        for w in range(half):
            for n in range(2 * length):
                here_now = jnp.logical_and(at == w, i == n)
                value = jnp.where(here_now, order[w][n][k], value)
        return value

    for load in loads[1:]:
        load.wait()

    def step_of(i, carry):
        run_slot(i, 0)
        zz = place(lookup(i, 0))
        xx = (x + lookup(i, 1)) % 2
        partner_copy(zz, xx).wait_recv()
        inner(zz, xx)
        run_slot(i, 1)
        outer(zz, xx)
        answer_copy(zz, xx).start()
        return carry

    lax.fori_loop(0, 2 * length, step_of, 0)
    run_slot(None, 0)

    for step in range(1, members):
        weights_copy(step).wait_send()
    for w in range(half):

        @pl.when(at == w)
        def _(w=w):
            counts = {}
            for kind, u, col, way, n in sent[w]:
                counts[kind, u, col, way] = counts.get((kind, u, col, way), 0) + n
            for (kind, u, col, way), n in counts.items():
                zz, xx = place(u), column(col)
                if kind == "t":
                    token_copy(zz, xx, 0, way, n).wait_send()
                elif kind == "x":
                    over_copy(zz, xx, 0, n).wait_send()
                else:
                    flow_copy(zz, xx, 0, way, n).wait_send()

    def drain(zz, carry):
        for xx in range(2):
            partner_copy(zz, xx).wait_send()
            answer_copy(zz, xx).wait_send()
        return carry

    lax.fori_loop(0, length, drain, 0)


def gathered_plan(tokens, expert_ids, combine, gate_proj, up_proj, down_proj, capacity):
    members = lax.axis_size("ep")
    here, features = tokens.shape
    ff = gate_proj.shape[1]
    length = members // 4
    pieces = max(n for n in range(1, PIECES + 1) if features % (16 * n) == 0)
    routes = Routes(length, pieces, TWIN, NEAR, *ORDER)
    block = (features, here)
    dma = pltpu.SemaphoreType.DMA
    vmem = lambda *shape: pltpu.VMEM(shape, jnp.bfloat16)
    anywhere = pl.BlockSpec(memory_space=pl.ANY)
    inside = pl.BlockSpec(memory_space=pltpu.VMEM)
    return pl.pallas_call(
        functools.partial(
            exchange_kernel, members=members, capacity=capacity, routes=routes
        ),
        out_shape=jax.ShapeDtypeStruct(block, jnp.bfloat16),
        in_specs=[inside, inside, anywhere, anywhere, anywhere, anywhere],
        out_specs=inside,
        scratch_shapes=[
            vmem(length, 2, 2, *block),
            pltpu.VMEM((members, 1, here), jnp.float32),
            pltpu.VMEM((members, 1, here), jnp.float32),
            pltpu.VMEM((members, 1, here), jnp.float32),
            vmem(features, ff), vmem(features, ff), vmem(ff, features),
            vmem(2 * capacity, ff),
            vmem(length, 2, 2, *block), vmem(length, 2, *block),
            vmem(length, *block), vmem(2, length, 2, *block),
            dma((4,)), dma((length, 2, 3)), dma((length, 2)), dma((members,)),
            dma((length, 2)), dma((length, 2, 2)),
            dma((length, 2, pieces)), dma((length, 2)), dma((members,)), dma((length, 2)),
            dma((length, pieces)), dma((2, length, 2, pieces)),
        ],
        compiler_params=pltpu.CompilerParams(
            collective_id=0, has_side_effects=True, vmem_limit_bytes=60 * 1024 * 1024
        ),
    )(expert_ids.T, combine.T, tokens.T, gate_proj, up_proj, down_proj).T


def on_device(tokens, expert_ids, combine, gate_weight, up_weight, down_weight):
    members = lax.axis_size("ep")
    tokens_here, fanout = expert_ids.shape
    features = tokens.shape[1]
    capacity = 2 * tokens_here * fanout // members
    received_rows = members * capacity
    if members % 4 == 0 and 2 * capacity >= tokens_here:
        return gathered_plan(
            tokens, expert_ids, combine, gate_weight[0], up_weight[0], down_weight[0], capacity
        )
    flat_ids = expert_ids.reshape(-1)
    onehot = (flat_ids[:, None] == jnp.arange(members, dtype=jnp.int32)[None, :]).astype(jnp.int32)
    running = jnp.cumsum(onehot, axis=0) - onehot
    slot_rank = jnp.sum(running * onehot, axis=1)
    target = flat_ids * capacity + slot_rank
    source_token = jnp.arange(tokens_here * fanout, dtype=jnp.int32) // fanout
    outgoing = (
        jnp.zeros((received_rows, features), jnp.bfloat16).at[target].set(tokens[source_token])
    )
    outgoing = outgoing.reshape(members, capacity, features)
    gate_proj, up_proj, down_proj = (gate_weight[0], up_weight[0], down_weight[0])
    arrived = lax.all_to_all(outgoing, "ep", split_axis=0, concat_axis=0, tiled=True)
    shape_here = arrived.shape
    answers = run_expert_block(
        arrived.reshape(-1, features), gate_proj, up_proj, down_proj
    ).reshape(shape_here)
    returned = lax.all_to_all(answers, "ep", split_axis=0, concat_axis=0, tiled=True)
    selected_experts = (
        returned.reshape(-1, features)[target]
        .astype(jnp.float32)
        .reshape(tokens_here, fanout, features)
    )
    mixture = jnp.sum(selected_experts * combine[:, :, None], axis=1)
    return mixture.astype(jnp.bfloat16)


def solution(mesh):
    in_specs = (
        P(("groups", "ep"), None),
        P(("groups", "ep"), None),
        P(("groups", "ep"), None),
        P("ep", None, None),
        P("ep", None, None),
        P("ep", None, None),
    )
    out_specs = P(("groups", "ep"), None)
    return jax.shard_map(
        on_device, mesh=mesh, in_specs=in_specs, out_specs=out_specs, check_vma=False
    )
```

```python
import functools

import jax
import jax.numpy as jnp
from jax import lax
from jax.experimental import pallas as pl
from jax.experimental.pallas import tpu as pltpu
from jax.sharding import PartitionSpec as P

MESH = pl.DeviceIdType.MESH

alpha_gate = 1.702

PIECES, PARTS = 7, 6
TWIN, NEAR = ((0.67, 0.5, 0.17), (0.17, 0), (0,)), ((0.83, 0.33, 0.33), (0.67, 0.67), (0,))
ORDER = ((1.0, 0.33), 1, True, ((0, 5), (0, 0)), ((0, 1, 4, 2, 3, 6, 5, 7), (2, 3, 0, 4, 1, 5, 7, 6)), ((1, 4, 1, 1, 2, 2, 3, 3), (2, 1, 4, 4, 3, 1, 2, 2)))
CHUNKS = (1.8, 0.9)
HOP, ACROSS_CHIP, BLOCK = 2.4, 1.6, 8.0


def run_expert_block(row_block, gate_proj, up_proj, down_proj):
    gate_part = jnp.dot(row_block, gate_proj, preferred_element_type=jnp.float32)
    up_part = jnp.dot(row_block, up_proj, preferred_element_type=jnp.float32)
    hidden = ((up_part + 1.0) * gate_part * jax.nn.sigmoid(alpha_gate * gate_part)).astype(
        jnp.bfloat16
    )
    return jnp.dot(hidden, down_proj, preferred_element_type=jnp.float32).astype(jnp.bfloat16)


class Routes:
    def __init__(self, length, pieces, parts, twin, near, first, crossing, far, after, pairs, urgency):
        self.length, self.pieces, self.parts = length, pieces, parts
        self.half = (length + 1) // 2
        self.shares = twin, near
        self.first, self.crossing, self.far = first, crossing, far
        self.after, self.pairs, self.urgency = after, pairs, urgency

    def within(self, which, u, w, distance, p):
        if u >= self.half:
            u, w = self.length - 1 - u, self.length - 1 - w
        kind = 0 if u == 0 else 1 if w > u else 2
        shares = self.shares[which][kind]
        count = self.parts if which else self.pieces
        return p < shares[min(distance, len(shares)) - 1] * count - 0.5

    def twin(self, u, w, distance, p):
        return self.within(0, u, w, distance, p)

    def near(self, u, w, distance, q):
        return self.within(1, u, w, distance, q)

    def exists(self, w, d):
        return 0 <= w + d < self.length

    def late(self, w, p, d):
        share = self.first[d < 0]
        return p >= share * self.pieces - 0.5 and w > 0 and w + 1 < self.length

    def crosses_late(self, p):
        return p >= self.crossing * self.pieces - 0.5

    def neighbour(self, w, d):
        to = w + d
        return (to, False) if to < self.half else (self.length - 1 - to, True)

    def token_moves(self, w, u, col, p):
        if u == w:
            ways = tuple(d for d in (1, -1) if self.exists(w, d))
            if col == 0:
                early = tuple(d for d in ways if not self.late(w, p, d))
                return early, not self.crosses_late(p)
            return tuple(d for d in ways if self.twin(w, w + d, 1, p)), False
        d, far = (1, w - u) if u < w else (-1, u - w)
        onward = self.exists(w, d)
        if col == 0:
            return ((d,) if onward else ()), not self.twin(u, w, far, p)
        if not self.twin(u, w, far, p):
            return (), False
        return ((d,) if onward and self.twin(u, w, far + 1, p) else ()), False

    def sum_inputs(self, kind, w, u, col, q):
        if kind == "X":
            return (), False
        if kind == "Z":
            d, away = (1, u - w) if u > w else (-1, w - u)
            chains = self.exists(w, -d) and (col == 0 or self.near(u, w, away + 1, q))
            return ((d,) if chains else ()), not self.near(u, w, away, q)
        chains = tuple(
            d for d in (1, -1)
            if self.exists(w, -d) and (col == 0 or self.near(w, w - d, 1, q))
        )
        return chains, col == 0


def make_plan(routes):
    length, pieces, half = routes.length, routes.pieces, routes.half
    parts = routes.parts
    never = 1e9
    token_wire, sum_wire = BLOCK / pieces, BLOCK / parts
    link, tok, pair_in, ans, cross, chain = {}, {}, {}, {}, {}, {}
    done_at = [dict() for _ in range(half)]

    def push(w, name, now, wire=token_wire):
        start = max(now, link.get((w, name), 0.0))
        link[w, name] = start + wire
        return start + wire + HOP

    def send_tokens(w, u, col, p, now):
        moves, crosses = routes.token_moves(w, u, col, p)
        for d in moves:
            to, mirrored = routes.neighbour(w, d)
            tok[to, length - 1 - u if mirrored else u, col, p] = push(w, d, now)
        if crosses:
            tok[w, u, 1 - col, p] = push(w, 0, now)
        key = (w, u, col)
        pair_in.setdefault(key, {})[p] = now + ACROSS_CHIP

    def send_sum(kind, w, u, col, q, now):
        if kind == "X" or (kind == "F" and col == 1):
            cross[w, u, q] = push(w, 0, now, sum_wire)
        elif kind == "Z":
            d = 1 if u > w else -1
            to, mirrored = routes.neighbour(w, d)
            key = (to, -d, length - 1 - u) if mirrored else (to, d, u)
            chain[key + (col, q)] = push(w, d, now, sum_wire)

    todo = []
    for w in range(half):
        ops = []
        for u in range(length):
            for col in range(2):
                if (u, col) == (w, 0):
                    ops += [("o", u, 0, p) for p in range(pieces) if routes.late(w, p, -1)]
                    ops += [("v", u, 0, p) for p in range(pieces) if routes.late(w, p, 1)]
                    ops += [("c", u, 0, p) for p in range(pieces) if routes.crosses_late(p)]
                else:
                    ops += [("t", u, col, p) for p in range(pieces)]
            for q in range(parts):
                if u == w:
                    ops += [("F", u, 1, q), ("F", u, 0, q)]
                elif routes.near(u, w, abs(u - w), q):
                    ops += [("Z", u, 0, q), ("Z", u, 1, q)]
                else:
                    ops += [("X", u, 1, q), ("Z", u, 0, q)]
        todo.append(ops)

    def ready_at(w, op):
        kind, u, col, p = op
        if kind == "t":
            return tok.get((w, u, col, p), never)
        if kind == "o":
            return never if any(o[:3] == ("t", length - 1, 0) for o in todo[w]) else 0.0
        if kind == "v":
            return never if any(o[0] == "t" and o[1] < w and o[2] == 0 for o in todo[w]) else 0.0
        if kind == "c":
            waiting = any(
                o[0] == "t" and routes.token_moves(w, *o[1:])[1] for o in todo[w]
            )
            return never if waiting else 0.0
        at = ans.get((w, u, col), never)
        if kind == "X" or (kind == "F" and col == 1):
            at = max(at, routes.after[w][kind == "F"])
        chains, crossing = routes.sum_inputs(kind, w, u, col, p)
        for d in chains:
            at = max(at, chain.get((w, d, u, col, p), never))
        if crossing:
            at = max(at, cross.get((w, u, p), never))
        return at

    pairs = []
    for w in range(half):
        wanted = sorted(
            ((u, col) for u in range(length) for col in range(2)),
            key=lambda k: (abs(k[0] - w), k[1], k[0]),
        )
        if length == len(routes.pairs[w]) // 2:
            wanted = [(n // 2, n % 2) for n in routes.pairs[w]]
        pairs.append(wanted)

    def precedence(w, op):
        kind, u, col, p = op
        if kind in "tocv":
            return -1, (-1 if routes.far else 1) * abs(u - w), u, col, p
        n = 2 * u + col
        rank = routes.urgency[w][n] if 2 * length == len(routes.urgency[w]) else abs(u - w)
        return rank, kind != "X", u, col, p

    order = [[] for _ in range(half)]
    slots = [{} for _ in range(half)]
    busy = [0.0] * half
    at_slot = [(0, 0)] * half
    running = [None] * half
    for w in range(half):
        for p in range(pieces):
            send_tokens(w, w, 0, p, 0.0)
    steps = 2 * length
    tick, now, end = 0.1, 0.0, [0.0] * half
    while now < 1000 and any(todo):
        for w in range(half):
            if busy[w] > now:
                continue
            if running[w] is not None:
                u, col = running[w]
                ans[w, u, col] = now + ACROSS_CHIP
                running[w] = None
            open_ops, held = [], set()
            for op in todo[w]:
                lane = op[:3]
                if lane in held:
                    continue
                if ready_at(w, op) <= now:
                    open_ops.append(op)
                elif op[0] == "t":
                    held.add(lane)
            i, j = at_slot[w]
            if open_ops:
                op = min(open_ops, key=lambda o: precedence(w, o))
                todo[w].remove(op)
                slots[w].setdefault((i, j), []).append(op)
                kind = op[0]
                busy[w] = now + (0.05 if kind in "tocv" else 0.4 / parts + 0.05)
                if kind == "t":
                    send_tokens(w, *op[1:], now)
                elif kind in "ov":
                    way = -1 if kind == "o" else 1
                    to, mirrored = routes.neighbour(w, way)
                    tok[to, length - 1 - w if mirrored else w, 0, op[3]] = push(w, way, now)
                elif kind == "c":
                    tok[w, w, 1, op[3]] = push(w, 0, now)
                else:
                    send_sum(kind, w, *op[1:], busy[w])
                end[w] = busy[w]
                continue
            if i < steps:
                if j == 0:
                    got = [
                        k for k in pairs[w]
                        if len(pair_in.get((w,) + k, {})) == pieces
                        and max(pair_in[(w,) + k].values()) <= now
                    ]
                    if not got or now < 2.5:
                        continue
                    pairs[w].remove(got[0])
                    order[w].append(got[0])
                busy[w] = now + CHUNKS[j]
                if j + 1 == len(CHUNKS):
                    running[w] = order[w][-1]
                    at_slot[w] = (i + 1, 0)
                else:
                    at_slot[w] = (i, j + 1)
        now += tick
    return order, slots, end


def grouped(routes, w, ops):
    groups = []
    for kind, u, col, p in ops:
        if kind in "ocv":
            how = {"o": ((-1,), False), "v": ((1,), False), "c": ((), True)}[kind]
        elif kind == "t":
            how = routes.token_moves(w, u, col, p)
        else:
            how = routes.sum_inputs(kind, w, u, col, p)
        if groups and groups[-1][:4] == [kind, u, col, how] and groups[-1][5] == p:
            groups[-1][5] = p + 1
        else:
            groups.append([kind, u, col, how, p, p + 1])
    return groups


def exchange_kernel(
    ids_hbm, share_hbm, tok_hbm, gate_hbm, up_hbm, down_hbm, out_ref,
    ids_ref, share_ref, x_buf, gate_w, up_w, down_w, hid, mixer, sums, quad, over, flow,
    load_sem, x_s, xp_s, q_s, sum_s, x_r, xp_r, q_r, over_r, flow_r,
    *, members, capacity, routes,
):
    length, pieces, half = routes.length, routes.pieces, routes.half
    order, slots, _ = make_plan(routes)
    features, here = tok_hbm.shape
    deep = x_buf.shape[3]
    size, span = deep // pieces, features // routes.parts
    me = lax.axis_index("ep")
    z, x, c = me // 4, (me // 2) % 2, me % 2
    flip = 2 * z >= length
    at = jnp.where(flip, length - 1 - z, z)

    def member(zz, xx, cc):
        return (zz * 2 + xx) * 2 + cc

    across, partner = member(z, 1 - x, c), member(z, x, 1 - c)
    step_up = jnp.where(flip, -1, 1)

    def beside(d):
        return member(jnp.clip(z + d * step_up, 0, length - 1), x, c)

    def lane(d):
        return jnp.where(flip, 1, 0) if d > 0 else jnp.where(flip, 0, 1)

    def place(u):
        return jnp.where(flip, length - 1 - u, u)

    def column(col):
        return x if col == 0 else 1 - x

    def cut(p, count=1):
        return pl.ds(pl.multiple_of(p * size, size), count * size)

    def stretch(q, count=1):
        return pl.ds(pl.multiple_of(q * span, span), count * span)

    def send(src, dst, ssem, rsem, to):
        return pltpu.make_async_remote_copy(
            src_ref=src, dst_ref=dst, send_sem=ssem, recv_sem=rsem,
            device_id={"ep": to}, device_id_type=MESH,
        )

    def each(p0, p1, act):
        if p1 - p0 == 1:
            act(p0)
            return

        def one(p, carry):
            act(p)
            return carry

        lax.fori_loop(p0, p1, one, 0)

    loads = [
        pltpu.make_async_copy(tok_hbm, x_buf.at[z, x, c, pl.ds(0, features)], load_sem.at[0]),
        pltpu.make_async_copy(gate_hbm, gate_w, load_sem.at[1]),
        pltpu.make_async_copy(up_hbm, up_w, load_sem.at[2]),
        pltpu.make_async_copy(down_hbm, down_w, load_sem.at[3]),
    ]
    lists = [
        pltpu.make_async_copy(ids_hbm, ids_ref, load_sem.at[4]),
        pltpu.make_async_copy(share_hbm, share_ref, load_sem.at[5]),
    ]
    for load in lists + loads:
        load.start()

    barrier = pltpu.get_barrier_semaphore()
    above, below = z < length - 1, z > 0

    def greet(to):
        pl.semaphore_signal(barrier, inc=1, device_id={"ep": to}, device_id_type=MESH)

    greet(partner)
    greet(across)

    @pl.when(above)
    def _():
        greet(member(z + 1, x, c))

    @pl.when(below)
    def _():
        greet(member(z - 1, x, c))

    for load in lists:
        load.wait()
    table = deep - features
    expert = lax.broadcasted_iota(jnp.int32, (table, here), 0)
    mix = jnp.zeros((table, here), jnp.float32)
    for k in range(ids_ref.shape[0]):
        mix += jnp.where(ids_ref[k : k + 1, :] == expert, share_ref[k : k + 1, :], 0.0)
    x_buf[z, x, c, features:deep, :] = mix.astype(jnp.bfloat16)
    pl.semaphore_wait(barrier, 2 + jnp.where(above, 1, 0) + jnp.where(below, 1, 0))

    sent = [[] for _ in range(half)]

    def token_copy(zz, xx, p, way, count=1):
        slot = x_buf.at[zz, xx, c, cut(p, count)]
        number, to = (2, across) if way == 0 else (lane(way), beside(way))
        return send(slot, slot, x_s.at[zz, xx, number], x_r.at[zz, xx, p], to)

    def partner_copy(zz, xx, p=None):
        slot = x_buf.at[zz, xx, c] if p is None else x_buf.at[zz, xx, c, cut(p)]
        return send(slot, slot, xp_s.at[zz, xx], xp_r.at[zz, xx], partner)

    def move_tokens(w, u, col, how, p0, p1, arriving, share=True):
        zz, xx = place(u), column(col)
        ways = tuple(how[0]) + ((0,) if how[1] else ())

        def one(p):
            if arriving:
                token_copy(zz, xx, p, 0).wait_recv()
            for way in ways:
                token_copy(zz, xx, p, way).start()
            if share:
                partner_copy(zz, xx, p).start()

        each(p0, p1, one)
        for way in ways:
            sent[w].append(("t", u, col, way, p1 - p0))

    joins = [{} for _ in range(half)]
    for w in range(half):
        for slot in sorted(slots[w]):
            for kind, u, col, q in slots[w][slot]:
                if kind in "XZF":
                    joins[w].setdefault((u, col), (kind, q))

    def answer_copy(zz, xx):
        return send(
            sums.at[zz, xx, 1 - c], quad.at[zz, xx], q_s.at[zz, xx], q_r.at[zz, xx], partner
        )

    def over_copy(zz, xx, q, count=1):
        return send(
            sums.at[zz, xx, c, stretch(q, count)], over.at[zz, stretch(q, count)],
            sum_s.at[zz, xx, 0], over_r.at[zz, q], across,
        )

    def flow_copy(zz, xx, q, way, count=1):
        d = lane(way)
        return send(
            sums.at[zz, xx, c, stretch(q, count)], flow.at[d, zz, xx, stretch(q, count)],
            sum_s.at[zz, xx, 1], flow_r.at[d, zz, xx, q], beside(way),
        )

    def move_sums(kind, w, u, col, how, q0, q1):
        zz, xx = place(u), column(col)
        chains, crossing = how
        if joins[w][u, col] == (kind, q0):
            answer_copy(zz, xx).wait_recv()
        leaves = kind == "X" or (kind == "F" and col == 1)
        onward = 1 if u > w else -1

        def one(q):
            for d in chains:
                flow_copy(zz, xx, q, d).wait_recv()
            if crossing:
                over_copy(zz, xx, q).wait_recv()
            total = sums[zz, xx, c, stretch(q)].astype(jnp.float32)
            total += quad[zz, xx, stretch(q)].astype(jnp.float32)
            if crossing:
                total += over[zz, stretch(q)].astype(jnp.float32)
            for d in chains:
                total += flow[lane(d), zz, xx, stretch(q)].astype(jnp.float32)
            total = total.astype(jnp.bfloat16)
            if kind == "F" and col == 0:
                out_ref[stretch(q), :] = total
                return
            sums[zz, xx, c, stretch(q)] = total
            if leaves:
                over_copy(zz, xx, q).start()
            else:
                flow_copy(zz, xx, q, onward).start()

        each(q0, q1, one)
        if leaves:
            sent[w].append(("x", u, col, 0, q1 - q0))
        elif kind == "Z":
            sent[w].append(("z", u, col, onward, q1 - q0))

    def run_slot(i, j):
        for w in range(half):
            due = [(k, slots[w][k, j]) for k in range(2 * length + 1) if (k, j) in slots[w]]
            due = [(k, ops) for k, ops in due if (k == 2 * length) == (i is None)]
            if not due:
                continue

            @pl.when(at == w)
            def _(w=w, due=due):
                for k, ops in due:

                    def act(ops=ops):
                        for kind, u, col, how, p0, p1 in grouped(routes, w, ops):
                            if kind == "t":
                                move_tokens(w, u, col, how, p0, p1, True)
                            elif kind in "ocv":
                                move_tokens(w, u, col, how, p0, p1, False, False)
                            else:
                                move_sums(kind, w, u, col, how, p0, p1)

                    if i is None:
                        act()
                    else:
                        pl.when(i == k)(act)

    loads[0].wait()
    for w in range(half):

        @pl.when(at == w)
        def _(w=w):
            for _, u, col, how, p0, p1 in grouped(
                routes, w, [("t", w, 0, p) for p in range(pieces)]
            ):
                move_tokens(w, u, col, how, p0, p1, False)

    before = (
        lax.broadcasted_iota(jnp.int32, (here, here), 0)
        < lax.broadcasted_iota(jnp.int32, (here, here), 1)
    ).astype(jnp.bfloat16)
    row_at = lax.broadcasted_iota(jnp.int32, (capacity, here), 0).astype(jnp.float32)

    def pickers(zz, xx):
        weights = []
        for cc in range(2):
            listed = x_buf[zz, xx, cc, features:deep, :].astype(jnp.float32)
            weights.append(jnp.sum(jnp.where(expert == me, listed, 0.0), axis=0, keepdims=True))
        line = lax.broadcasted_iota(jnp.int32, (16, here), 0)
        flags = jnp.where(line == 0, weights[0], jnp.where(line == 1, weights[1], 0.0)) > 0.0
        rank = jnp.dot(
            flags.astype(jnp.float32).astype(jnp.bfloat16), before,
            preferred_element_type=jnp.float32,
        )
        none = jnp.zeros((capacity, here), jnp.bfloat16)
        picks = []
        for cc in range(2):
            named = weights[cc] > 0.0
            pick = jnp.where(named, rank[cc : cc + 1, :], -1.0) == row_at
            picks.append((
                pick.astype(jnp.float32).astype(jnp.bfloat16),
                jnp.where(pick, weights[cc], 0.0).astype(jnp.bfloat16),
            ))

        def spread(k):
            first = jnp.concatenate([picks[0][k], none], axis=1)
            second = jnp.concatenate([none, picks[1][k]], axis=1)
            return jnp.concatenate([first, second], axis=0)

        return spread(0), spread(1)

    def inner(zz, xx):
        pick, mixer[...] = pickers(zz, xx)
        pair = jnp.concatenate(
            [x_buf[zz, xx, 0, :features, :], x_buf[zz, xx, 1, :features, :]], axis=1
        )
        block = lax.dot_general(
            pick, pair, (((1,), (1,)), ((), ())), preferred_element_type=jnp.float32
        ).astype(jnp.bfloat16)
        gate = jnp.dot(block, gate_w[...], preferred_element_type=jnp.float32)
        up = jnp.dot(block, up_w[...], preferred_element_type=jnp.float32)
        hid[...] = ((up + 1.0) * gate * jax.nn.sigmoid(alpha_gate * gate)).astype(jnp.bfloat16)

    def outer(zz, xx):
        answer = jnp.dot(
            hid[...], down_w[...], preferred_element_type=jnp.float32
        ).astype(jnp.bfloat16)
        back = lax.dot_general(
            answer, mixer[...], (((0,), (0,)), ((), ())), preferred_element_type=jnp.float32
        ).astype(jnp.bfloat16)
        for cc in range(2):
            sums[zz, xx, cc] = back[:, cc * here : (cc + 1) * here]

    def lookup(i, k):
        value = 0
        for w in range(half):
            for n in range(2 * length):
                here_now = jnp.logical_and(at == w, i == n)
                value = jnp.where(here_now, order[w][n][k], value)
        return value

    for load in loads[1:]:
        load.wait()

    def step_of(i, carry):
        run_slot(i, 0)
        zz = place(lookup(i, 0))
        xx = (x + lookup(i, 1)) % 2
        partner_copy(zz, xx).wait_recv()
        inner(zz, xx)
        run_slot(i, 1)
        outer(zz, xx)
        answer_copy(zz, xx).start()
        return carry

    lax.fori_loop(0, 2 * length, step_of, 0)
    run_slot(None, 0)

    for w in range(half):

        @pl.when(at == w)
        def _(w=w):
            counts = {}
            for kind, u, col, way, n in sent[w]:
                counts[kind, u, col, way] = counts.get((kind, u, col, way), 0) + n
            for (kind, u, col, way), n in counts.items():
                zz, xx = place(u), column(col)
                if kind == "t":
                    token_copy(zz, xx, 0, way, n).wait_send()
                elif kind == "x":
                    over_copy(zz, xx, 0, n).wait_send()
                else:
                    flow_copy(zz, xx, 0, way, n).wait_send()

    def drain(zz, carry):
        for xx in range(2):
            partner_copy(zz, xx).wait_send()
            answer_copy(zz, xx).wait_send()
        return carry

    lax.fori_loop(0, length, drain, 0)


def gathered_plan(tokens, expert_ids, combine, gate_proj, up_proj, down_proj, capacity):
    members = lax.axis_size("ep")
    here, features = tokens.shape
    ff = gate_proj.shape[1]
    length = members // 4
    deep = features + -(-members // 16) * 16
    pieces = max(n for n in range(1, PIECES + 1) if deep % (16 * n) == 0)
    parts = max(n for n in range(1, PARTS + 1) if features % (16 * n) == 0)
    routes = Routes(length, pieces, parts, TWIN, NEAR, *ORDER)
    block = (features, here)
    dma = pltpu.SemaphoreType.DMA
    vmem = lambda *shape: pltpu.VMEM(shape, jnp.bfloat16)
    anywhere = pl.BlockSpec(memory_space=pl.ANY)
    inside = pl.BlockSpec(memory_space=pltpu.VMEM)
    return pl.pallas_call(
        functools.partial(
            exchange_kernel, members=members, capacity=capacity, routes=routes
        ),
        out_shape=jax.ShapeDtypeStruct(block, jnp.bfloat16),
        in_specs=[anywhere, anywhere, anywhere, anywhere, anywhere, anywhere],
        out_specs=inside,
        scratch_shapes=[
            pltpu.VMEM(expert_ids.shape[::-1], jnp.int32),
            pltpu.VMEM(combine.shape[::-1], jnp.float32),
            vmem(length, 2, 2, deep, here),
            vmem(features, ff), vmem(features, ff), vmem(ff, features),
            vmem(2 * capacity, ff), vmem(2 * capacity, 2 * here),
            vmem(length, 2, 2, *block), vmem(length, 2, *block),
            vmem(length, *block), vmem(2, length, 2, *block),
            dma((6,)), dma((length, 2, 3)), dma((length, 2)),
            dma((length, 2)), dma((length, 2, 2)),
            dma((length, 2, pieces)), dma((length, 2)), dma((length, 2)),
            dma((length, parts)), dma((2, length, 2, parts)),
        ],
        compiler_params=pltpu.CompilerParams(
            collective_id=0, has_side_effects=True, vmem_limit_bytes=60 * 1024 * 1024
        ),
    )(expert_ids.T, combine.T, tokens.T, gate_proj, up_proj, down_proj).T


def on_device(tokens, expert_ids, combine, gate_weight, up_weight, down_weight):
    members = lax.axis_size("ep")
    tokens_here, fanout = expert_ids.shape
    features = tokens.shape[1]
    capacity = 2 * tokens_here * fanout // members
    received_rows = members * capacity
    if members % 4 == 0 and 2 * capacity >= tokens_here:
        return gathered_plan(
            tokens, expert_ids, combine, gate_weight[0], up_weight[0], down_weight[0], capacity
        )
    flat_ids = expert_ids.reshape(-1)
    onehot = (flat_ids[:, None] == jnp.arange(members, dtype=jnp.int32)[None, :]).astype(jnp.int32)
    running = jnp.cumsum(onehot, axis=0) - onehot
    slot_rank = jnp.sum(running * onehot, axis=1)
    target = flat_ids * capacity + slot_rank
    source_token = jnp.arange(tokens_here * fanout, dtype=jnp.int32) // fanout
    outgoing = (
        jnp.zeros((received_rows, features), jnp.bfloat16).at[target].set(tokens[source_token])
    )
    outgoing = outgoing.reshape(members, capacity, features)
    gate_proj, up_proj, down_proj = (gate_weight[0], up_weight[0], down_weight[0])
    arrived = lax.all_to_all(outgoing, "ep", split_axis=0, concat_axis=0, tiled=True)
    shape_here = arrived.shape
    answers = run_expert_block(
        arrived.reshape(-1, features), gate_proj, up_proj, down_proj
    ).reshape(shape_here)
    returned = lax.all_to_all(answers, "ep", split_axis=0, concat_axis=0, tiled=True)
    selected_experts = (
        returned.reshape(-1, features)[target]
        .astype(jnp.float32)
        .reshape(tokens_here, fanout, features)
    )
    mixture = jnp.sum(selected_experts * combine[:, :, None], axis=1)
    return mixture.astype(jnp.bfloat16)


def solution(mesh):
    in_specs = (
        P(("groups", "ep"), None),
        P(("groups", "ep"), None),
        P(("groups", "ep"), None),
        P("ep", None, None),
        P("ep", None, None),
        P("ep", None, None),
    )
    out_specs = P(("groups", "ep"), None)
    return jax.shard_map(
        on_device, mesh=mesh, in_specs=in_specs, out_specs=out_specs, check_vma=False
    )
```

```python
import functools

import jax
import jax.numpy as jnp
from jax import lax
from jax.experimental import pallas as pl
from jax.experimental.pallas import tpu as pltpu
from jax.sharding import PartitionSpec as P

MESH = pl.DeviceIdType.MESH

alpha_gate = 1.702

PIECES, PARTS = 7, 9
TWIN, NEAR = ((0.56, 0.44, 0), (0, 0), (0,)), ((0.33, 0.33, 0.33), (0.22, 0.11), (0.89,))
ORDER = ((0.33, 1.0), 0.56, True, ((8, 37), (5, 0)), ((0, 3, 4, 7, 2, 6, 1, 5), (2, 6, 5, 0, 3, 1, 7, 4)), ((0, 0, 3, 0, 2, 4, 3, 1), (2, 1, 0, 3, 4, 3, 2, 4)), (12, 12))
CHUNKS = (1.8, 0.9)
HOP, ACROSS_CHIP, BLOCK = 2.4, 1.6, 8.0


def run_expert_block(row_block, gate_proj, up_proj, down_proj):
    gate_part = jnp.dot(row_block, gate_proj, preferred_element_type=jnp.float32)
    up_part = jnp.dot(row_block, up_proj, preferred_element_type=jnp.float32)
    hidden = ((up_part + 1.0) * gate_part * jax.nn.sigmoid(alpha_gate * gate_part)).astype(
        jnp.bfloat16
    )
    return jnp.dot(hidden, down_proj, preferred_element_type=jnp.float32).astype(jnp.bfloat16)


class Routes:
    def __init__(self, length, pieces, parts, twin, near, first, crossing, far, after, pairs, urgency, quota):
        self.length, self.pieces, self.parts = length, pieces, parts
        self.half = (length + 1) // 2
        self.shares = twin, near
        self.first, self.crossing, self.far = first, crossing, far
        self.after, self.pairs, self.urgency = after, pairs, urgency
        self.quota = quota

    def within(self, which, u, w, distance, p):
        if u >= self.half:
            u, w = self.length - 1 - u, self.length - 1 - w
        kind = 0 if u == 0 else 1 if w > u else 2
        shares = self.shares[which][kind]
        count = self.parts if which else self.pieces
        return p < shares[min(distance, len(shares)) - 1] * count - 0.5

    def twin(self, u, w, distance, p):
        return self.within(0, u, w, distance, p)

    def near(self, u, w, distance, q):
        return self.within(1, u, w, distance, q)

    def exists(self, w, d):
        return 0 <= w + d < self.length

    def late(self, w, p, d):
        share = self.first[d < 0]
        return p >= share * self.pieces - 0.5 and w > 0 and w + 1 < self.length

    def crosses_late(self, p):
        return p >= self.crossing * self.pieces - 0.5

    def neighbour(self, w, d):
        to = w + d
        return (to, False) if to < self.half else (self.length - 1 - to, True)

    def token_moves(self, w, u, col, p):
        if u == w:
            ways = tuple(d for d in (1, -1) if self.exists(w, d))
            if col == 0:
                early = tuple(d for d in ways if not self.late(w, p, d))
                return early, not self.crosses_late(p)
            return tuple(d for d in ways if self.twin(w, w + d, 1, p)), False
        d, far = (1, w - u) if u < w else (-1, u - w)
        onward = self.exists(w, d)
        if col == 0:
            return ((d,) if onward else ()), not self.twin(u, w, far, p)
        if not self.twin(u, w, far, p):
            return (), False
        return ((d,) if onward and self.twin(u, w, far + 1, p) else ()), False

    def sum_inputs(self, kind, w, u, col, q):
        if kind == "X":
            return (), False
        if kind == "Z":
            d, away = (1, u - w) if u > w else (-1, w - u)
            chains = self.exists(w, -d) and (col == 0 or self.near(u, w, away + 1, q))
            return ((d,) if chains else ()), not self.near(u, w, away, q)
        chains = tuple(
            d for d in (1, -1)
            if self.exists(w, -d) and (col == 0 or self.near(w, w - d, 1, q))
        )
        return chains, col == 0


def make_plan(routes):
    length, pieces, half = routes.length, routes.pieces, routes.half
    parts = routes.parts
    never = 1e9
    token_wire, sum_wire = BLOCK / pieces, BLOCK / parts
    link, tok, pair_in, ans, cross, chain = {}, {}, {}, {}, {}, {}
    done_at = [dict() for _ in range(half)]

    def push(w, name, now, wire=token_wire):
        start = max(now, link.get((w, name), 0.0))
        link[w, name] = start + wire
        return start + wire + HOP

    def send_tokens(w, u, col, p, now):
        moves, crosses = routes.token_moves(w, u, col, p)
        for d in moves:
            to, mirrored = routes.neighbour(w, d)
            tok[to, length - 1 - u if mirrored else u, col, p] = push(w, d, now)
        if crosses:
            tok[w, u, 1 - col, p] = push(w, 0, now)
        key = (w, u, col)
        pair_in.setdefault(key, {})[p] = now + ACROSS_CHIP

    def send_sum(kind, w, u, col, q, now):
        if kind == "X" or (kind == "F" and col == 1):
            cross[w, u, q] = push(w, 0, now, sum_wire)
        elif kind == "Z":
            d = 1 if u > w else -1
            to, mirrored = routes.neighbour(w, d)
            key = (to, -d, length - 1 - u) if mirrored else (to, d, u)
            chain[key + (col, q)] = push(w, d, now, sum_wire)

    todo = []
    for w in range(half):
        ops = []
        for u in range(length):
            for col in range(2):
                if (u, col) == (w, 0):
                    ops += [("o", u, 0, p) for p in range(pieces) if routes.late(w, p, -1)]
                    ops += [("v", u, 0, p) for p in range(pieces) if routes.late(w, p, 1)]
                    ops += [("c", u, 0, p) for p in range(pieces) if routes.crosses_late(p)]
                else:
                    ops += [("t", u, col, p) for p in range(pieces)]
            for q in range(parts):
                if u == w:
                    ops += [("F", u, 1, q), ("F", u, 0, q)]
                elif routes.near(u, w, abs(u - w), q):
                    ops += [("Z", u, 0, q), ("Z", u, 1, q)]
                else:
                    ops += [("X", u, 1, q), ("Z", u, 0, q)]
        todo.append(ops)

    def ready_at(w, op):
        kind, u, col, p = op
        if kind == "t":
            return tok.get((w, u, col, p), never)
        if kind == "o":
            return never if any(o[:3] == ("t", length - 1, 0) for o in todo[w]) else 0.0
        if kind == "v":
            return never if any(o[0] == "t" and o[1] < w and o[2] == 0 for o in todo[w]) else 0.0
        if kind == "c":
            waiting = any(
                o[0] == "t" and routes.token_moves(w, *o[1:])[1] for o in todo[w]
            )
            return never if waiting else 0.0
        at = ans.get((w, u, col), never)
        if kind == "X" or (kind == "F" and col == 1):
            at = max(at, routes.after[w][kind == "F"])
        chains, crossing = routes.sum_inputs(kind, w, u, col, p)
        for d in chains:
            at = max(at, chain.get((w, d, u, col, p), never))
        if crossing:
            at = max(at, cross.get((w, u, p), never))
        return at

    pairs = []
    for w in range(half):
        wanted = sorted(
            ((u, col) for u in range(length) for col in range(2)),
            key=lambda k: (abs(k[0] - w), k[1], k[0]),
        )
        if length == len(routes.pairs[w]) // 2:
            wanted = [(n // 2, n % 2) for n in routes.pairs[w]]
        pairs.append(wanted)

    def precedence(w, op):
        kind, u, col, p = op
        if kind in "tocv":
            return -1, (-1 if routes.far else 1) * abs(u - w), u, col, p
        n = 2 * u + col
        rank = routes.urgency[w][n] if 2 * length == len(routes.urgency[w]) else abs(u - w)
        return rank, kind != "X", u, col, p

    order = [[] for _ in range(half)]
    slots = [{} for _ in range(half)]
    busy = [0.0] * half
    at_slot = [(0, 0)] * half
    running = [None] * half
    for w in range(half):
        for p in range(pieces):
            send_tokens(w, w, 0, p, 0.0)
    steps = 2 * length
    tick, now, end = 0.1, 0.0, [0.0] * half
    while now < 1000 and any(todo):
        for w in range(half):
            if busy[w] > now:
                continue
            if running[w] is not None:
                u, col = running[w]
                ans[w, u, col] = now + ACROSS_CHIP
                running[w] = None
            open_ops, held = [], set()
            for op in todo[w]:
                lane = op[:3]
                if lane in held:
                    continue
                if ready_at(w, op) <= now:
                    open_ops.append(op)
                elif op[0] == "t":
                    held.add(lane)
            i, j = at_slot[w]
            got = []
            if i < steps and j == 0 and now >= 2.5:
                got = [
                    k for k in pairs[w]
                    if len(pair_in.get((w,) + k, {})) == pieces
                    and max(pair_in[(w,) + k].values()) <= now
                ]
            quota = routes.quota[w] if i < steps and (j > 0 or got) else never
            sums_here = sum(o[0] in "XZF" for o in slots[w].get((i, j), ()))
            if sums_here >= quota:
                open_ops = [o for o in open_ops if o[0] in "tocv"]
            if open_ops:
                op = min(open_ops, key=lambda o: precedence(w, o))
                todo[w].remove(op)
                slots[w].setdefault((i, j), []).append(op)
                kind = op[0]
                busy[w] = now + (0.05 if kind in "tocv" else 0.4 / parts + 0.05)
                if kind == "t":
                    send_tokens(w, *op[1:], now)
                elif kind in "ov":
                    way = -1 if kind == "o" else 1
                    to, mirrored = routes.neighbour(w, way)
                    tok[to, length - 1 - w if mirrored else w, 0, op[3]] = push(w, way, now)
                elif kind == "c":
                    tok[w, w, 1, op[3]] = push(w, 0, now)
                else:
                    send_sum(kind, w, *op[1:], busy[w])
                end[w] = busy[w]
                continue
            if i < steps:
                if j == 0:
                    if not got:
                        continue
                    pairs[w].remove(got[0])
                    order[w].append(got[0])
                busy[w] = now + CHUNKS[j]
                if j + 1 == len(CHUNKS):
                    running[w] = order[w][-1]
                    at_slot[w] = (i + 1, 0)
                else:
                    at_slot[w] = (i, j + 1)
        now += tick
    return order, slots, end


def grouped(routes, w, ops):
    groups = []
    for kind, u, col, p in ops:
        if kind in "ocv":
            how = {"o": ((-1,), False), "v": ((1,), False), "c": ((), True)}[kind]
        elif kind == "t":
            how = routes.token_moves(w, u, col, p)
        else:
            how = routes.sum_inputs(kind, w, u, col, p)
        if groups and groups[-1][:4] == [kind, u, col, how] and groups[-1][5] == p:
            groups[-1][5] = p + 1
        else:
            groups.append([kind, u, col, how, p, p + 1])
    return groups


def exchange_kernel(
    ids_hbm, share_hbm, tok_hbm, gate_hbm, up_hbm, down_hbm, out_hbm,
    ids_ref, share_ref, x_buf, gate_w, up_w, down_w, hid, mixer, sums, quad, over, flow, result,
    load_sem, x_s, xp_s, q_s, sum_s, x_r, xp_r, q_r, over_r, flow_r, out_s,
    *, members, capacity, routes,
):
    length, pieces, half = routes.length, routes.pieces, routes.half
    order, slots, _ = make_plan(routes)
    features, here = tok_hbm.shape
    deep = x_buf.shape[3]
    size, span = deep // pieces, features // routes.parts
    me = lax.axis_index("ep")
    z, x, c = me // 4, (me // 2) % 2, me % 2
    flip = 2 * z >= length
    at = jnp.where(flip, length - 1 - z, z)

    def member(zz, xx, cc):
        return (zz * 2 + xx) * 2 + cc

    across, partner = member(z, 1 - x, c), member(z, x, 1 - c)
    step_up = jnp.where(flip, -1, 1)

    def beside(d):
        return member(jnp.clip(z + d * step_up, 0, length - 1), x, c)

    def lane(d):
        return jnp.where(flip, 1, 0) if d > 0 else jnp.where(flip, 0, 1)

    def place(u):
        return jnp.where(flip, length - 1 - u, u)

    def column(col):
        return x if col == 0 else 1 - x

    def cut(p, count=1):
        return pl.ds(pl.multiple_of(p * size, size), count * size)

    def stretch(q, count=1):
        return pl.ds(pl.multiple_of(q * span, span), count * span)

    def send(src, dst, ssem, rsem, to):
        return pltpu.make_async_remote_copy(
            src_ref=src, dst_ref=dst, send_sem=ssem, recv_sem=rsem,
            device_id={"ep": to}, device_id_type=MESH,
        )

    def each(p0, p1, act):
        if p1 - p0 == 1:
            act(p0)
            return

        def one(p, carry):
            act(p)
            return carry

        lax.fori_loop(p0, p1, one, 0)

    loads = [
        pltpu.make_async_copy(tok_hbm, x_buf.at[z, x, c, pl.ds(0, features)], load_sem.at[0]),
        pltpu.make_async_copy(gate_hbm, gate_w, load_sem.at[1]),
        pltpu.make_async_copy(up_hbm, up_w, load_sem.at[2]),
        pltpu.make_async_copy(down_hbm, down_w, load_sem.at[3]),
    ]
    lists = [
        pltpu.make_async_copy(ids_hbm, ids_ref, load_sem.at[4]),
        pltpu.make_async_copy(share_hbm, share_ref, load_sem.at[5]),
    ]
    for load in lists + loads:
        load.start()

    barrier = pltpu.get_barrier_semaphore()
    above, below = z < length - 1, z > 0

    def greet(to):
        pl.semaphore_signal(barrier, inc=1, device_id={"ep": to}, device_id_type=MESH)

    greet(partner)
    greet(across)

    @pl.when(above)
    def _():
        greet(member(z + 1, x, c))

    @pl.when(below)
    def _():
        greet(member(z - 1, x, c))

    for load in lists:
        load.wait()
    table = deep - features
    expert = lax.broadcasted_iota(jnp.int32, (table, here), 0)
    mix = jnp.zeros((table, here), jnp.float32)
    for k in range(ids_ref.shape[0]):
        mix += jnp.where(ids_ref[k : k + 1, :] == expert, share_ref[k : k + 1, :], 0.0)
    x_buf[z, x, c, features:deep, :] = mix.astype(jnp.bfloat16)
    pl.semaphore_wait(barrier, 2 + jnp.where(above, 1, 0) + jnp.where(below, 1, 0))

    sent = [[] for _ in range(half)]

    def token_copy(zz, xx, p, way, count=1):
        slot = x_buf.at[zz, xx, c, cut(p, count)]
        number, to = (2, across) if way == 0 else (lane(way), beside(way))
        return send(slot, slot, x_s.at[zz, xx, number], x_r.at[zz, xx, p], to)

    def partner_copy(zz, xx, p=None):
        slot = x_buf.at[zz, xx, c] if p is None else x_buf.at[zz, xx, c, cut(p)]
        return send(slot, slot, xp_s.at[zz, xx], xp_r.at[zz, xx], partner)

    def move_tokens(w, u, col, how, p0, p1, arriving, share=True):
        zz, xx = place(u), column(col)
        ways = tuple(how[0]) + ((0,) if how[1] else ())

        def one(p):
            if arriving:
                token_copy(zz, xx, p, 0).wait_recv()
            for way in ways:
                token_copy(zz, xx, p, way).start()
            if share:
                partner_copy(zz, xx, p).start()

        each(p0, p1, one)
        for way in ways:
            sent[w].append(("t", u, col, way, p1 - p0))

    joins = [{} for _ in range(half)]
    for w in range(half):
        for slot in sorted(slots[w]):
            for kind, u, col, q in slots[w][slot]:
                if kind in "XZF":
                    joins[w].setdefault((u, col), (kind, q))

    def answer_copy(zz, xx):
        return send(
            sums.at[zz, xx, 1 - c], quad.at[zz, xx], q_s.at[zz, xx], q_r.at[zz, xx], partner
        )

    def result_copy(q):
        return pltpu.make_async_copy(
            result.at[stretch(q)], out_hbm.at[stretch(q)], out_s.at[q]
        )

    def over_copy(zz, xx, q, count=1):
        return send(
            sums.at[zz, xx, c, stretch(q, count)], over.at[zz, stretch(q, count)],
            sum_s.at[zz, xx, 0], over_r.at[zz, q], across,
        )

    def flow_copy(zz, xx, q, way, count=1):
        d = lane(way)
        return send(
            sums.at[zz, xx, c, stretch(q, count)], flow.at[d, zz, xx, stretch(q, count)],
            sum_s.at[zz, xx, 1], flow_r.at[d, zz, xx, q], beside(way),
        )

    def move_sums(kind, w, u, col, how, q0, q1):
        zz, xx = place(u), column(col)
        chains, crossing = how
        if joins[w][u, col] == (kind, q0):
            answer_copy(zz, xx).wait_recv()
        leaves = kind == "X" or (kind == "F" and col == 1)
        onward = 1 if u > w else -1

        def one(q):
            for d in chains:
                flow_copy(zz, xx, q, d).wait_recv()
            if crossing:
                over_copy(zz, xx, q).wait_recv()
            total = sums[zz, xx, c, stretch(q)].astype(jnp.float32)
            total += quad[zz, xx, stretch(q)].astype(jnp.float32)
            if crossing:
                total += over[zz, stretch(q)].astype(jnp.float32)
            for d in chains:
                total += flow[lane(d), zz, xx, stretch(q)].astype(jnp.float32)
            total = total.astype(jnp.bfloat16)
            if kind == "F" and col == 0:
                result[stretch(q), :] = total
                result_copy(q).start()
                return
            sums[zz, xx, c, stretch(q)] = total
            if leaves:
                over_copy(zz, xx, q).start()
            else:
                flow_copy(zz, xx, q, onward).start()

        each(q0, q1, one)
        if leaves:
            sent[w].append(("x", u, col, 0, q1 - q0))
        elif kind == "Z":
            sent[w].append(("z", u, col, onward, q1 - q0))

    def run_slot(i, j):
        for w in range(half):
            due = [(k, slots[w][k, j]) for k in range(2 * length + 1) if (k, j) in slots[w]]
            due = [(k, ops) for k, ops in due if (k == 2 * length) == (i is None)]
            if not due:
                continue

            @pl.when(at == w)
            def _(w=w, due=due):
                for k, ops in due:

                    def act(ops=ops):
                        for kind, u, col, how, p0, p1 in grouped(routes, w, ops):
                            if kind == "t":
                                move_tokens(w, u, col, how, p0, p1, True)
                            elif kind in "ocv":
                                move_tokens(w, u, col, how, p0, p1, False, False)
                            else:
                                move_sums(kind, w, u, col, how, p0, p1)

                    if i is None:
                        act()
                    else:
                        pl.when(i == k)(act)

    loads[0].wait()
    for w in range(half):

        @pl.when(at == w)
        def _(w=w):
            for _, u, col, how, p0, p1 in grouped(
                routes, w, [("t", w, 0, p) for p in range(pieces)]
            ):
                move_tokens(w, u, col, how, p0, p1, False)

    before = (
        lax.broadcasted_iota(jnp.int32, (here, here), 0)
        < lax.broadcasted_iota(jnp.int32, (here, here), 1)
    ).astype(jnp.bfloat16)
    row_at = lax.broadcasted_iota(jnp.int32, (capacity, here), 0).astype(jnp.float32)

    def pickers(zz, xx):
        weights = []
        for cc in range(2):
            listed = x_buf[zz, xx, cc, features:deep, :].astype(jnp.float32)
            weights.append(jnp.sum(jnp.where(expert == me, listed, 0.0), axis=0, keepdims=True))
        line = lax.broadcasted_iota(jnp.int32, (16, here), 0)
        flags = jnp.where(line == 0, weights[0], jnp.where(line == 1, weights[1], 0.0)) > 0.0
        rank = jnp.dot(
            flags.astype(jnp.float32).astype(jnp.bfloat16), before,
            preferred_element_type=jnp.float32,
        )
        none = jnp.zeros((capacity, here), jnp.bfloat16)
        picks = []
        for cc in range(2):
            named = weights[cc] > 0.0
            pick = jnp.where(named, rank[cc : cc + 1, :], -1.0) == row_at
            picks.append((
                pick.astype(jnp.float32).astype(jnp.bfloat16),
                jnp.where(pick, weights[cc], 0.0).astype(jnp.bfloat16),
            ))

        def spread(k):
            first = jnp.concatenate([picks[0][k], none], axis=1)
            second = jnp.concatenate([none, picks[1][k]], axis=1)
            return jnp.concatenate([first, second], axis=0)

        return spread(0), spread(1)

    def inner(zz, xx):
        pick, mixer[...] = pickers(zz, xx)
        pair = jnp.concatenate(
            [x_buf[zz, xx, 0, :features, :], x_buf[zz, xx, 1, :features, :]], axis=1
        )
        block = lax.dot_general(
            pick, pair, (((1,), (1,)), ((), ())), preferred_element_type=jnp.float32
        ).astype(jnp.bfloat16)
        gate = jnp.dot(block, gate_w[...], preferred_element_type=jnp.float32)
        up = jnp.dot(block, up_w[...], preferred_element_type=jnp.float32)
        hid[...] = ((up + 1.0) * gate * jax.nn.sigmoid(alpha_gate * gate)).astype(jnp.bfloat16)

    def outer(zz, xx):
        answer = jnp.dot(
            hid[...], down_w[...], preferred_element_type=jnp.float32
        ).astype(jnp.bfloat16)
        back = lax.dot_general(
            answer, mixer[...], (((0,), (0,)), ((), ())), preferred_element_type=jnp.float32
        ).astype(jnp.bfloat16)
        for cc in range(2):
            sums[zz, xx, cc] = back[:, cc * here : (cc + 1) * here]

    def lookup(i, k):
        value = 0
        for w in range(half):
            for n in range(2 * length):
                here_now = jnp.logical_and(at == w, i == n)
                value = jnp.where(here_now, order[w][n][k], value)
        return value

    for load in loads[1:]:
        load.wait()

    def step_of(i, carry):
        run_slot(i, 0)
        zz = place(lookup(i, 0))
        xx = (x + lookup(i, 1)) % 2
        partner_copy(zz, xx).wait_recv()
        inner(zz, xx)
        run_slot(i, 1)
        outer(zz, xx)
        answer_copy(zz, xx).start()
        return carry

    lax.fori_loop(0, 2 * length, step_of, 0)
    run_slot(None, 0)

    for w in range(half):

        @pl.when(at == w)
        def _(w=w):
            counts = {}
            for kind, u, col, way, n in sent[w]:
                counts[kind, u, col, way] = counts.get((kind, u, col, way), 0) + n
            for (kind, u, col, way), n in counts.items():
                zz, xx = place(u), column(col)
                if kind == "t":
                    token_copy(zz, xx, 0, way, n).wait_send()
                elif kind == "x":
                    over_copy(zz, xx, 0, n).wait_send()
                else:
                    flow_copy(zz, xx, 0, way, n).wait_send()

    def drain(zz, carry):
        for xx in range(2):
            partner_copy(zz, xx).wait_send()
            answer_copy(zz, xx).wait_send()
        return carry

    lax.fori_loop(0, length, drain, 0)
    for q in range(routes.parts):
        result_copy(q).wait()


def gathered_plan(tokens, expert_ids, combine, gate_proj, up_proj, down_proj, capacity):
    members = lax.axis_size("ep")
    here, features = tokens.shape
    ff = gate_proj.shape[1]
    length = members // 4
    deep = features + -(-members // 16) * 16
    pieces = max(n for n in range(1, PIECES + 1) if deep % (16 * n) == 0)
    parts = max(n for n in range(1, PARTS + 1) if features % (16 * n) == 0)
    routes = Routes(length, pieces, parts, TWIN, NEAR, *ORDER)
    block = (features, here)
    dma = pltpu.SemaphoreType.DMA
    vmem = lambda *shape: pltpu.VMEM(shape, jnp.bfloat16)
    anywhere = pl.BlockSpec(memory_space=pl.ANY)
    return pl.pallas_call(
        functools.partial(
            exchange_kernel, members=members, capacity=capacity, routes=routes
        ),
        out_shape=jax.ShapeDtypeStruct(block, jnp.bfloat16),
        in_specs=[anywhere, anywhere, anywhere, anywhere, anywhere, anywhere],
        out_specs=anywhere,
        scratch_shapes=[
            pltpu.VMEM(expert_ids.shape[::-1], jnp.int32),
            pltpu.VMEM(combine.shape[::-1], jnp.float32),
            vmem(length, 2, 2, deep, here),
            vmem(features, ff), vmem(features, ff), vmem(ff, features),
            vmem(2 * capacity, ff), vmem(2 * capacity, 2 * here),
            vmem(length, 2, 2, *block), vmem(length, 2, *block),
            vmem(length, *block), vmem(2, length, 2, *block), vmem(*block),
            dma((6,)), dma((length, 2, 3)), dma((length, 2)),
            dma((length, 2)), dma((length, 2, 2)),
            dma((length, 2, pieces)), dma((length, 2)), dma((length, 2)),
            dma((length, parts)), dma((2, length, 2, parts)), dma((parts,)),
        ],
        compiler_params=pltpu.CompilerParams(
            collective_id=0, has_side_effects=True, vmem_limit_bytes=60 * 1024 * 1024
        ),
    )(expert_ids.T, combine.T, tokens.T, gate_proj, up_proj, down_proj).T


def on_device(tokens, expert_ids, combine, gate_weight, up_weight, down_weight):
    members = lax.axis_size("ep")
    tokens_here, fanout = expert_ids.shape
    features = tokens.shape[1]
    capacity = 2 * tokens_here * fanout // members
    received_rows = members * capacity
    if members % 4 == 0 and 2 * capacity >= tokens_here:
        return gathered_plan(
            tokens, expert_ids, combine, gate_weight[0], up_weight[0], down_weight[0], capacity
        )
    flat_ids = expert_ids.reshape(-1)
    onehot = (flat_ids[:, None] == jnp.arange(members, dtype=jnp.int32)[None, :]).astype(jnp.int32)
    running = jnp.cumsum(onehot, axis=0) - onehot
    slot_rank = jnp.sum(running * onehot, axis=1)
    target = flat_ids * capacity + slot_rank
    source_token = jnp.arange(tokens_here * fanout, dtype=jnp.int32) // fanout
    outgoing = (
        jnp.zeros((received_rows, features), jnp.bfloat16).at[target].set(tokens[source_token])
    )
    outgoing = outgoing.reshape(members, capacity, features)
    gate_proj, up_proj, down_proj = (gate_weight[0], up_weight[0], down_weight[0])
    arrived = lax.all_to_all(outgoing, "ep", split_axis=0, concat_axis=0, tiled=True)
    shape_here = arrived.shape
    answers = run_expert_block(
        arrived.reshape(-1, features), gate_proj, up_proj, down_proj
    ).reshape(shape_here)
    returned = lax.all_to_all(answers, "ep", split_axis=0, concat_axis=0, tiled=True)
    selected_experts = (
        returned.reshape(-1, features)[target]
        .astype(jnp.float32)
        .reshape(tokens_here, fanout, features)
    )
    mixture = jnp.sum(selected_experts * combine[:, :, None], axis=1)
    return mixture.astype(jnp.bfloat16)


def solution(mesh):
    in_specs = (
        P(("groups", "ep"), None),
        P(("groups", "ep"), None),
        P(("groups", "ep"), None),
        P("ep", None, None),
        P("ep", None, None),
        P("ep", None, None),
    )
    out_specs = P(("groups", "ep"), None)
    return jax.shard_map(
        on_device, mesh=mesh, in_specs=in_specs, out_specs=out_specs, check_vma=False
    )
```

```python
import functools

import jax
import jax.numpy as jnp
from jax import lax
from jax.experimental import pallas as pl
from jax.experimental.pallas import tpu as pltpu
from jax.sharding import PartitionSpec as P

MESH = pl.DeviceIdType.MESH

alpha_gate = 1.702

PIECES, PARTS = 7, 9
TWIN, NEAR = ((0.56, 0.44, 0), (0, 0), (0,)), ((0.33, 0.33, 0.33), (0.22, 0.11), (0.89,))
ORDER = ((0.33, 1.0), 0.56, True, ((8, 37), (5, 0)), ((0, 3, 4, 7, 2, 6, 1, 5), (2, 6, 5, 0, 3, 1, 7, 4)), ((0, 0, 3, 0, 2, 4, 3, 1), (2, 1, 0, 3, 4, 3, 2, 4)), (12, 12))
CHUNKS = (1.8, 0.9)
HOP, ACROSS_CHIP, BLOCK = 2.4, 1.6, 8.0


def run_expert_block(row_block, gate_proj, up_proj, down_proj):
    gate_part = jnp.dot(row_block, gate_proj, preferred_element_type=jnp.float32)
    up_part = jnp.dot(row_block, up_proj, preferred_element_type=jnp.float32)
    hidden = ((up_part + 1.0) * gate_part * jax.nn.sigmoid(alpha_gate * gate_part)).astype(
        jnp.bfloat16
    )
    return jnp.dot(hidden, down_proj, preferred_element_type=jnp.float32).astype(jnp.bfloat16)


class Routes:
    def __init__(self, length, pieces, parts, twin, near, first, crossing, far, after, pairs, urgency, quota):
        self.length, self.pieces, self.parts = length, pieces, parts
        self.half = (length + 1) // 2
        self.shares = twin, near
        self.first, self.crossing, self.far = first, crossing, far
        self.after, self.pairs, self.urgency = after, pairs, urgency
        self.quota = quota

    def within(self, which, u, w, distance, p):
        if u >= self.half:
            u, w = self.length - 1 - u, self.length - 1 - w
        kind = 0 if u == 0 else 1 if w > u else 2
        shares = self.shares[which][kind]
        count = self.parts if which else self.pieces
        return p < shares[min(distance, len(shares)) - 1] * count - 0.5

    def twin(self, u, w, distance, p):
        return self.within(0, u, w, distance, p)

    def near(self, u, w, distance, q):
        return self.within(1, u, w, distance, q)

    def exists(self, w, d):
        return 0 <= w + d < self.length

    def late(self, w, p, d):
        share = self.first[d < 0]
        return p >= share * self.pieces - 0.5 and w > 0 and w + 1 < self.length

    def crosses_late(self, p):
        return p >= self.crossing * self.pieces - 0.5

    def neighbour(self, w, d):
        to = w + d
        return (to, False) if to < self.half else (self.length - 1 - to, True)

    def token_moves(self, w, u, col, p):
        if u == w:
            ways = tuple(d for d in (1, -1) if self.exists(w, d))
            if col == 0:
                early = tuple(d for d in ways if not self.late(w, p, d))
                return early, not self.crosses_late(p)
            return tuple(d for d in ways if self.twin(w, w + d, 1, p)), False
        d, far = (1, w - u) if u < w else (-1, u - w)
        onward = self.exists(w, d)
        if col == 0:
            return ((d,) if onward else ()), not self.twin(u, w, far, p)
        if not self.twin(u, w, far, p):
            return (), False
        return ((d,) if onward and self.twin(u, w, far + 1, p) else ()), False

    def sum_inputs(self, kind, w, u, col, q):
        if kind == "X":
            return (), False
        if kind == "Z":
            d, away = (1, u - w) if u > w else (-1, w - u)
            chains = self.exists(w, -d) and (col == 0 or self.near(u, w, away + 1, q))
            return ((d,) if chains else ()), not self.near(u, w, away, q)
        chains = tuple(
            d for d in (1, -1)
            if self.exists(w, -d) and (col == 0 or self.near(w, w - d, 1, q))
        )
        return chains, col == 0


def make_plan(routes):
    length, pieces, half = routes.length, routes.pieces, routes.half
    parts = routes.parts
    never = 1e9
    token_wire, sum_wire = BLOCK / pieces, BLOCK / parts
    link, tok, pair_in, ans, cross, chain = {}, {}, {}, {}, {}, {}
    done_at = [dict() for _ in range(half)]

    def push(w, name, now, wire=token_wire):
        start = max(now, link.get((w, name), 0.0))
        link[w, name] = start + wire
        return start + wire + HOP

    def send_tokens(w, u, col, p, now):
        moves, crosses = routes.token_moves(w, u, col, p)
        for d in moves:
            to, mirrored = routes.neighbour(w, d)
            tok[to, length - 1 - u if mirrored else u, col, p] = push(w, d, now)
        if crosses:
            tok[w, u, 1 - col, p] = push(w, 0, now)
        key = (w, u, col)
        pair_in.setdefault(key, {})[p] = now + ACROSS_CHIP

    def send_sum(kind, w, u, col, q, now):
        if kind == "X" or (kind == "F" and col == 1):
            cross[w, u, q] = push(w, 0, now, sum_wire)
        elif kind == "Z":
            d = 1 if u > w else -1
            to, mirrored = routes.neighbour(w, d)
            key = (to, -d, length - 1 - u) if mirrored else (to, d, u)
            chain[key + (col, q)] = push(w, d, now, sum_wire)

    todo = []
    for w in range(half):
        ops = []
        for u in range(length):
            for col in range(2):
                if (u, col) == (w, 0):
                    ops += [("o", u, 0, p) for p in range(pieces) if routes.late(w, p, -1)]
                    ops += [("v", u, 0, p) for p in range(pieces) if routes.late(w, p, 1)]
                    ops += [("c", u, 0, p) for p in range(pieces) if routes.crosses_late(p)]
                else:
                    ops += [("t", u, col, p) for p in range(pieces)]
            for q in range(parts):
                if u == w:
                    ops += [("F", u, 1, q), ("F", u, 0, q)]
                elif routes.near(u, w, abs(u - w), q):
                    ops += [("Z", u, 0, q), ("Z", u, 1, q)]
                else:
                    ops += [("X", u, 1, q), ("Z", u, 0, q)]
        todo.append(ops)

    def ready_at(w, op):
        kind, u, col, p = op
        if kind == "t":
            return tok.get((w, u, col, p), never)
        if kind == "o":
            return never if any(o[:3] == ("t", length - 1, 0) for o in todo[w]) else 0.0
        if kind == "v":
            return never if any(o[0] == "t" and o[1] < w and o[2] == 0 for o in todo[w]) else 0.0
        if kind == "c":
            waiting = any(
                o[0] == "t" and routes.token_moves(w, *o[1:])[1] for o in todo[w]
            )
            return never if waiting else 0.0
        at = ans.get((w, u, col), never)
        if kind == "X" or (kind == "F" and col == 1):
            at = max(at, routes.after[w][kind == "F"])
        chains, crossing = routes.sum_inputs(kind, w, u, col, p)
        for d in chains:
            at = max(at, chain.get((w, d, u, col, p), never))
        if crossing:
            at = max(at, cross.get((w, u, p), never))
        return at

    pairs = []
    for w in range(half):
        wanted = sorted(
            ((u, col) for u in range(length) for col in range(2)),
            key=lambda k: (abs(k[0] - w), k[1], k[0]),
        )
        if length == len(routes.pairs[w]) // 2:
            wanted = [(n // 2, n % 2) for n in routes.pairs[w]]
        pairs.append(wanted)

    def precedence(w, op):
        kind, u, col, p = op
        if kind in "tocv":
            return -1, (-1 if routes.far else 1) * abs(u - w), u, col, p
        n = 2 * u + col
        rank = routes.urgency[w][n] if 2 * length == len(routes.urgency[w]) else abs(u - w)
        return rank, kind != "X", u, col, p

    order = [[] for _ in range(half)]
    slots = [{} for _ in range(half)]
    busy = [0.0] * half
    at_slot = [(0, 0)] * half
    running = [None] * half
    for w in range(half):
        for p in range(pieces):
            send_tokens(w, w, 0, p, 0.0)
    steps = 2 * length
    tick, now, end = 0.1, 0.0, [0.0] * half
    while now < 1000 and any(todo):
        for w in range(half):
            if busy[w] > now:
                continue
            if running[w] is not None:
                u, col = running[w]
                ans[w, u, col] = now + ACROSS_CHIP
                running[w] = None
            open_ops, held = [], set()
            for op in todo[w]:
                lane = op[:3]
                if lane in held:
                    continue
                if ready_at(w, op) <= now:
                    open_ops.append(op)
                elif op[0] == "t":
                    held.add(lane)
            i, j = at_slot[w]
            got = []
            if i < steps and j == 0 and now >= 2.5:
                got = [
                    k for k in pairs[w]
                    if len(pair_in.get((w,) + k, {})) == pieces
                    and max(pair_in[(w,) + k].values()) <= now
                ]
            quota = routes.quota[w] if i < steps and (j > 0 or got) else never
            sums_here = sum(o[0] in "XZF" for o in slots[w].get((i, j), ()))
            if sums_here >= quota:
                open_ops = [o for o in open_ops if o[0] in "tocv"]
            if open_ops:
                op = min(open_ops, key=lambda o: precedence(w, o))
                todo[w].remove(op)
                slots[w].setdefault((i, j), []).append(op)
                kind = op[0]
                busy[w] = now + (0.05 if kind in "tocv" else 0.4 / parts + 0.05)
                if kind == "t":
                    send_tokens(w, *op[1:], now)
                elif kind in "ov":
                    way = -1 if kind == "o" else 1
                    to, mirrored = routes.neighbour(w, way)
                    tok[to, length - 1 - w if mirrored else w, 0, op[3]] = push(w, way, now)
                elif kind == "c":
                    tok[w, w, 1, op[3]] = push(w, 0, now)
                else:
                    send_sum(kind, w, *op[1:], busy[w])
                end[w] = busy[w]
                continue
            if i < steps:
                if j == 0:
                    if not got:
                        continue
                    pairs[w].remove(got[0])
                    order[w].append(got[0])
                busy[w] = now + CHUNKS[j]
                if j + 1 == len(CHUNKS):
                    running[w] = order[w][-1]
                    at_slot[w] = (i + 1, 0)
                else:
                    at_slot[w] = (i, j + 1)
        now += tick
    return order, slots, end


def grouped(routes, w, ops):
    groups = []
    for kind, u, col, p in ops:
        if kind in "ocv":
            how = {"o": ((-1,), False), "v": ((1,), False), "c": ((), True)}[kind]
        elif kind == "t":
            how = routes.token_moves(w, u, col, p)
        else:
            how = routes.sum_inputs(kind, w, u, col, p)
        if groups and groups[-1][:4] == [kind, u, col, how] and groups[-1][5] == p:
            groups[-1][5] = p + 1
        else:
            groups.append([kind, u, col, how, p, p + 1])
    return groups


def exchange_kernel(
    ids_hbm, share_hbm, tok_hbm, gate_hbm, up_hbm, down_hbm, out_hbm,
    ids_ref, share_ref, x_buf, gate_w, up_w, down_w, hid, mixer, sums, quad, over, flow, result,
    load_sem, x_s, xp_s, q_s, sum_s, x_r, xp_r, q_r, over_r, flow_r, out_s,
    *, members, capacity, routes,
):
    length, pieces, half = routes.length, routes.pieces, routes.half
    order, slots, _ = make_plan(routes)
    features, here = tok_hbm.shape
    deep = x_buf.shape[3]
    size, span = deep // pieces, features // routes.parts
    me = lax.axis_index("ep")
    z, x, c = me // 4, (me // 2) % 2, me % 2
    flip = 2 * z >= length
    at = jnp.where(flip, length - 1 - z, z)

    def member(zz, xx, cc):
        return (zz * 2 + xx) * 2 + cc

    across, partner = member(z, 1 - x, c), member(z, x, 1 - c)
    step_up = jnp.where(flip, -1, 1)

    def beside(d):
        return member(jnp.clip(z + d * step_up, 0, length - 1), x, c)

    def lane(d):
        return jnp.where(flip, 1, 0) if d > 0 else jnp.where(flip, 0, 1)

    def place(u):
        return jnp.where(flip, length - 1 - u, u)

    def column(col):
        return x if col == 0 else 1 - x

    def cut(p, count=1):
        return pl.ds(pl.multiple_of(p * size, size), count * size)

    def stretch(q, count=1):
        return pl.ds(pl.multiple_of(q * span, span), count * span)

    def send(src, dst, ssem, rsem, to):
        return pltpu.make_async_remote_copy(
            src_ref=src, dst_ref=dst, send_sem=ssem, recv_sem=rsem,
            device_id={"ep": to}, device_id_type=MESH,
        )

    def each(p0, p1, act):
        if p1 - p0 == 1:
            act(p0)
            return

        def one(p, carry):
            act(p)
            return carry

        lax.fori_loop(p0, p1, one, 0)

    loads = [
        pltpu.make_async_copy(tok_hbm, x_buf.at[z, x, c, pl.ds(0, features)], load_sem.at[0]),
        pltpu.make_async_copy(gate_hbm, gate_w, load_sem.at[1]),
        pltpu.make_async_copy(up_hbm, up_w, load_sem.at[2]),
        pltpu.make_async_copy(down_hbm, down_w, load_sem.at[3]),
    ]
    lists = [
        pltpu.make_async_copy(ids_hbm, ids_ref, load_sem.at[4]),
        pltpu.make_async_copy(share_hbm, share_ref, load_sem.at[5]),
    ]
    for load in lists + loads:
        load.start()

    barrier = pltpu.get_barrier_semaphore()
    above, below = z < length - 1, z > 0

    def greet(to):
        pl.semaphore_signal(barrier, inc=1, device_id={"ep": to}, device_id_type=MESH)

    greet(partner)
    greet(across)

    @pl.when(above)
    def _():
        greet(member(z + 1, x, c))

    @pl.when(below)
    def _():
        greet(member(z - 1, x, c))

    for load in lists:
        load.wait()
    table = deep - features
    expert = lax.broadcasted_iota(jnp.int32, (table, here), 0)
    mix = jnp.zeros((table, here), jnp.float32)
    for k in range(ids_ref.shape[0]):
        mix += jnp.where(ids_ref[k : k + 1, :] == expert, share_ref[k : k + 1, :], 0.0)
    x_buf[z, x, c, features:deep, :] = mix.astype(jnp.bfloat16)
    pl.semaphore_wait(barrier, 2 + jnp.where(above, 1, 0) + jnp.where(below, 1, 0))

    sent = [[] for _ in range(half)]

    def token_copy(zz, xx, p, way, count=1):
        slot = x_buf.at[zz, xx, c, cut(p, count)]
        number, to = (2, across) if way == 0 else (lane(way), beside(way))
        return send(slot, slot, x_s.at[zz, xx, number], x_r.at[zz, xx, p], to)

    def partner_copy(zz, xx, p=None):
        slot = x_buf.at[zz, xx, c] if p is None else x_buf.at[zz, xx, c, cut(p)]
        return send(slot, slot, xp_s.at[zz, xx], xp_r.at[zz, xx], partner)

    def move_tokens(w, u, col, how, p0, p1, arriving, share=True):
        zz, xx = place(u), column(col)
        ways = tuple(how[0]) + ((0,) if how[1] else ())

        def one(p):
            if arriving:
                token_copy(zz, xx, p, 0).wait_recv()
            for way in ways:
                token_copy(zz, xx, p, way).start()
            if share:
                partner_copy(zz, xx, p).start()

        each(p0, p1, one)
        for way in ways:
            sent[w].append(("t", u, col, way, p1 - p0))

    joins = [{} for _ in range(half)]
    for w in range(half):
        for slot in sorted(slots[w]):
            for kind, u, col, q in slots[w][slot]:
                if kind in "XZF":
                    joins[w].setdefault((u, col), (kind, q))

    def answer_copy(zz, xx):
        return send(
            sums.at[zz, xx, 1 - c], quad.at[zz, xx], q_s.at[zz, xx], q_r.at[zz, xx], partner
        )

    def result_copy(q):
        return pltpu.make_async_copy(
            result.at[stretch(q)], out_hbm.at[stretch(q)], out_s.at[q]
        )

    def over_copy(zz, xx, q, count=1):
        return send(
            sums.at[zz, xx, c, stretch(q, count)], over.at[zz, stretch(q, count)],
            sum_s.at[zz, xx, 0], over_r.at[zz, q], across,
        )

    def flow_copy(zz, xx, q, way, count=1):
        d = lane(way)
        return send(
            sums.at[zz, xx, c, stretch(q, count)], flow.at[d, zz, xx, stretch(q, count)],
            sum_s.at[zz, xx, 1], flow_r.at[d, zz, xx, q], beside(way),
        )

    def move_sums(kind, w, u, col, how, q0, q1):
        zz, xx = place(u), column(col)
        chains, crossing = how
        if joins[w][u, col] == (kind, q0):
            answer_copy(zz, xx).wait_recv()
        leaves = kind == "X" or (kind == "F" and col == 1)
        onward = 1 if u > w else -1

        def one(q):
            for d in chains:
                flow_copy(zz, xx, q, d).wait_recv()
            if crossing:
                over_copy(zz, xx, q).wait_recv()
            total = sums[zz, xx, c, stretch(q)].astype(jnp.float32)
            total += quad[zz, xx, stretch(q)].astype(jnp.float32)
            if crossing:
                total += over[zz, stretch(q)].astype(jnp.float32)
            for d in chains:
                total += flow[lane(d), zz, xx, stretch(q)].astype(jnp.float32)
            total = total.astype(jnp.bfloat16)
            if kind == "F" and col == 0:
                result[stretch(q), :] = total
                result_copy(q).start()
                return
            sums[zz, xx, c, stretch(q)] = total
            if leaves:
                over_copy(zz, xx, q).start()
            else:
                flow_copy(zz, xx, q, onward).start()

        each(q0, q1, one)
        if leaves:
            sent[w].append(("x", u, col, 0, q1 - q0))
        elif kind == "Z":
            sent[w].append(("z", u, col, onward, q1 - q0))

    def run_slot(i, j):
        for w in range(half):
            due = [(k, slots[w][k, j]) for k in range(2 * length + 1) if (k, j) in slots[w]]
            due = [(k, ops) for k, ops in due if (k == 2 * length) == (i is None)]
            if not due:
                continue

            @pl.when(at == w)
            def _(w=w, due=due):
                for k, ops in due:

                    def act(ops=ops):
                        for kind, u, col, how, p0, p1 in grouped(routes, w, ops):
                            if kind == "t":
                                move_tokens(w, u, col, how, p0, p1, True)
                            elif kind in "ocv":
                                move_tokens(w, u, col, how, p0, p1, False, False)
                            else:
                                move_sums(kind, w, u, col, how, p0, p1)

                    if i is None:
                        act()
                    else:
                        pl.when(i == k)(act)

    loads[0].wait()
    for w in range(half):

        @pl.when(at == w)
        def _(w=w):
            for _, u, col, how, p0, p1 in grouped(
                routes, w, [("t", w, 0, p) for p in range(pieces)]
            ):
                move_tokens(w, u, col, how, p0, p1, False)

    before = (
        lax.broadcasted_iota(jnp.int32, (here, here), 0)
        < lax.broadcasted_iota(jnp.int32, (here, here), 1)
    ).astype(jnp.bfloat16)
    row_at = lax.broadcasted_iota(jnp.int32, (capacity, here), 0).astype(jnp.float32)

    def pickers(zz, xx):
        weights = []
        for cc in range(2):
            listed = x_buf[zz, xx, cc, features:deep, :].astype(jnp.float32)
            weights.append(jnp.sum(jnp.where(expert == me, listed, 0.0), axis=0, keepdims=True))
        line = lax.broadcasted_iota(jnp.int32, (16, here), 0)
        flags = jnp.where(line == 0, weights[0], jnp.where(line == 1, weights[1], 0.0)) > 0.0
        rank = jnp.dot(
            flags.astype(jnp.float32).astype(jnp.bfloat16), before,
            preferred_element_type=jnp.float32,
        )
        none = jnp.zeros((capacity, here), jnp.bfloat16)
        picks = []
        for cc in range(2):
            named = weights[cc] > 0.0
            pick = jnp.where(named, rank[cc : cc + 1, :], -1.0) == row_at
            picks.append((
                pick.astype(jnp.float32).astype(jnp.bfloat16),
                jnp.where(pick, weights[cc], 0.0).astype(jnp.bfloat16),
            ))

        def spread(k):
            first = jnp.concatenate([picks[0][k], none], axis=1)
            second = jnp.concatenate([none, picks[1][k]], axis=1)
            return jnp.concatenate([first, second], axis=0)

        return spread(0), spread(1)

    def inner(zz, xx):
        pick, mixer[...] = pickers(zz, xx)
        pair = jnp.concatenate(
            [x_buf[zz, xx, 0, :features, :], x_buf[zz, xx, 1, :features, :]], axis=1
        )
        block = lax.dot_general(
            pick, pair, (((1,), (1,)), ((), ())), preferred_element_type=jnp.float32
        ).astype(jnp.bfloat16)
        gate = jnp.dot(block, gate_w[...], preferred_element_type=jnp.float32)
        up = jnp.dot(block, up_w[...], preferred_element_type=jnp.float32)
        hid[...] = ((up + 1.0) * gate * jax.nn.sigmoid(alpha_gate * gate)).astype(jnp.bfloat16)

    def outer(zz, xx):
        answer = jnp.dot(
            hid[...], down_w[...], preferred_element_type=jnp.float32
        ).astype(jnp.bfloat16)
        back = lax.dot_general(
            answer, mixer[...], (((0,), (0,)), ((), ())), preferred_element_type=jnp.float32
        ).astype(jnp.bfloat16)
        for cc in range(2):
            sums[zz, xx, cc] = back[:, cc * here : (cc + 1) * here]

    def lookup(i, k):
        value = 0
        for w in range(half):
            for n in range(2 * length):
                here_now = jnp.logical_and(at == w, i == n)
                value = jnp.where(here_now, order[w][n][k], value)
        return value

    for load in loads[1:3]:
        load.wait()

    def step_of(i, carry):
        run_slot(i, 0)
        zz = place(lookup(i, 0))
        xx = (x + lookup(i, 1)) % 2
        partner_copy(zz, xx).wait_recv()
        inner(zz, xx)
        run_slot(i, 1)
        pl.when(i == 0)(loads[3].wait)
        outer(zz, xx)
        answer_copy(zz, xx).start()
        return carry

    lax.fori_loop(0, 2 * length, step_of, 0)
    run_slot(None, 0)

    for w in range(half):

        @pl.when(at == w)
        def _(w=w):
            counts = {}
            for kind, u, col, way, n in sent[w]:
                counts[kind, u, col, way] = counts.get((kind, u, col, way), 0) + n
            for (kind, u, col, way), n in counts.items():
                zz, xx = place(u), column(col)
                if kind == "t":
                    token_copy(zz, xx, 0, way, n).wait_send()
                elif kind == "x":
                    over_copy(zz, xx, 0, n).wait_send()
                else:
                    flow_copy(zz, xx, 0, way, n).wait_send()

    def drain(zz, carry):
        for xx in range(2):
            partner_copy(zz, xx).wait_send()
            answer_copy(zz, xx).wait_send()
        return carry

    lax.fori_loop(0, length, drain, 0)
    for q in range(routes.parts):
        result_copy(q).wait()


def gathered_plan(tokens, expert_ids, combine, gate_proj, up_proj, down_proj, capacity):
    members = lax.axis_size("ep")
    here, features = tokens.shape
    ff = gate_proj.shape[1]
    length = members // 4
    deep = features + -(-members // 16) * 16
    pieces = max(n for n in range(1, PIECES + 1) if deep % (16 * n) == 0)
    parts = max(n for n in range(1, PARTS + 1) if features % (16 * n) == 0)
    routes = Routes(length, pieces, parts, TWIN, NEAR, *ORDER)
    block = (features, here)
    dma = pltpu.SemaphoreType.DMA
    vmem = lambda *shape: pltpu.VMEM(shape, jnp.bfloat16)
    anywhere = pl.BlockSpec(memory_space=pl.ANY)
    return pl.pallas_call(
        functools.partial(
            exchange_kernel, members=members, capacity=capacity, routes=routes
        ),
        out_shape=jax.ShapeDtypeStruct(block, jnp.bfloat16),
        in_specs=[anywhere, anywhere, anywhere, anywhere, anywhere, anywhere],
        out_specs=anywhere,
        scratch_shapes=[
            pltpu.VMEM(expert_ids.shape[::-1], jnp.int32),
            pltpu.VMEM(combine.shape[::-1], jnp.float32),
            vmem(length, 2, 2, deep, here),
            vmem(features, ff), vmem(features, ff), vmem(ff, features),
            vmem(2 * capacity, ff), vmem(2 * capacity, 2 * here),
            vmem(length, 2, 2, *block), vmem(length, 2, *block),
            vmem(length, *block), vmem(2, length, 2, *block), vmem(*block),
            dma((6,)), dma((length, 2, 3)), dma((length, 2)),
            dma((length, 2)), dma((length, 2, 2)),
            dma((length, 2, pieces)), dma((length, 2)), dma((length, 2)),
            dma((length, parts)), dma((2, length, 2, parts)), dma((parts,)),
        ],
        compiler_params=pltpu.CompilerParams(
            collective_id=0, has_side_effects=True, vmem_limit_bytes=60 * 1024 * 1024
        ),
    )(expert_ids.T, combine.T, tokens.T, gate_proj, up_proj, down_proj).T


def on_device(tokens, expert_ids, combine, gate_weight, up_weight, down_weight):
    members = lax.axis_size("ep")
    tokens_here, fanout = expert_ids.shape
    features = tokens.shape[1]
    capacity = 2 * tokens_here * fanout // members
    received_rows = members * capacity
    if members % 4 == 0 and 2 * capacity >= tokens_here:
        return gathered_plan(
            tokens, expert_ids, combine, gate_weight[0], up_weight[0], down_weight[0], capacity
        )
    flat_ids = expert_ids.reshape(-1)
    onehot = (flat_ids[:, None] == jnp.arange(members, dtype=jnp.int32)[None, :]).astype(jnp.int32)
    running = jnp.cumsum(onehot, axis=0) - onehot
    slot_rank = jnp.sum(running * onehot, axis=1)
    target = flat_ids * capacity + slot_rank
    source_token = jnp.arange(tokens_here * fanout, dtype=jnp.int32) // fanout
    outgoing = (
        jnp.zeros((received_rows, features), jnp.bfloat16).at[target].set(tokens[source_token])
    )
    outgoing = outgoing.reshape(members, capacity, features)
    gate_proj, up_proj, down_proj = (gate_weight[0], up_weight[0], down_weight[0])
    arrived = lax.all_to_all(outgoing, "ep", split_axis=0, concat_axis=0, tiled=True)
    shape_here = arrived.shape
    answers = run_expert_block(
        arrived.reshape(-1, features), gate_proj, up_proj, down_proj
    ).reshape(shape_here)
    returned = lax.all_to_all(answers, "ep", split_axis=0, concat_axis=0, tiled=True)
    selected_experts = (
        returned.reshape(-1, features)[target]
        .astype(jnp.float32)
        .reshape(tokens_here, fanout, features)
    )
    mixture = jnp.sum(selected_experts * combine[:, :, None], axis=1)
    return mixture.astype(jnp.bfloat16)


def solution(mesh):
    in_specs = (
        P(("groups", "ep"), None),
        P(("groups", "ep"), None),
        P(("groups", "ep"), None),
        P("ep", None, None),
        P("ep", None, None),
        P("ep", None, None),
    )
    out_specs = P(("groups", "ep"), None)
    return jax.shard_map(
        on_device, mesh=mesh, in_specs=in_specs, out_specs=out_specs, check_vma=False
    )
```
